512 devices in a mesh: dp: 32 (over z, y_hi), tensor: 16 (over x, y_lo, core).
Axes of the slice: x: 4, y: 8 (y_hi: 4, y_lo: 2; y = y_hi * 2 + y_lo), z: 8, core: 2. Of those that a mesh axis runs over, the one named last changes fastest.
Arguments:
- tokens_in: bfloat16 [4096, 4096], P(('dp', 'tensor')), may hold values from -6 to 6
- grad_out: bfloat16 [4096, 4096], P(('dp', 'tensor')), may hold values from -6 to 6
- gate_pre: bfloat16 [4096, 7168], P('dp', 'tensor'), may hold values from -6 to 6
- up_pre: bfloat16 [4096, 7168], P('dp', 'tensor'), may hold values from -6 to 6
- gate_weight: bfloat16 [4096, 7168], P('dp', 'tensor'), may hold values from -0.09375 to 0.09375
- up_weight: bfloat16 [4096, 7168], P('dp', 'tensor'), may hold values from -0.09375 to 0.09375
- down_weight: bfloat16 [7168, 4096], P('tensor', 'dp'), may hold values from -0.0625 to 0.0625
- norm_gain: float32 [4096], replicated, may hold values from 0.1 to 1.9
Outputs:
- input_grad: bfloat16 [4096, 4096], P(('dp', 'tensor'))
- gain_grad: float32 [4096], replicated
- down_grad: bfloat16 [7168, 4096], P('tensor', 'dp')
The draws below stay inside these ranges and needn't reach their ends.
All inputs are finite; a program needn't handle non-finite values.
Results may differ from the reference program's by a relative error of at most 0.015.
Values may be sent and summed in bfloat16 or wider, within the bound.
A program may use at most 64 MiB of HBM per device.

```python
import jax
import jax.numpy as jnp
from jax import lax

D = 4096
FF = 7168
TOKENS = 4096
N_TENSOR = 16


def block_levels(key, extent, shards, smallest, top_value):
    factor_of, own = 1.0, jax.random.fold_in(key, 6)
    for dim, parts in shards:
        heights = jnp.exp(jax.random.uniform(jax.random.fold_in(own, dim), (parts,), jnp.float32, smallest / len(shards), top_value / len(shards)))
        factor_of = factor_of * jnp.repeat(heights, extent[dim] // parts).reshape([-1 if axis == dim else 1 for axis in range(len(extent))])
    return factor_of


def gaussian(rng, dims, deviation, most, pieces=(), kind=jnp.bfloat16):
    array = jax.random.normal(rng, dims, jnp.float32) * deviation
    if len(pieces) > 0:
        array = block_levels(rng, dims, pieces, -0.22, 0.18) * array
    return jnp.clip(array, min=-most, max=most).astype(kind)


def setup_inputs(seed: int = 0) -> dict:
    keys = jax.random.split(jax.random.key(seed), 9)
    return {
        "tokens_in": gaussian(keys[0], (TOKENS, D), 1.0, 6.0, ((0, 512),)),
        "grad_out": gaussian(keys[1], (TOKENS, D), 1.0, 6.0, ((0, 512),)),
        "gate_pre": gaussian(keys[2], (TOKENS, FF), 1.0, 6.0, ((0, 32), (1, 16))),
        "up_pre": gaussian(keys[3], (TOKENS, FF), 1.0, 6.0, ((0, 32), (1, 16))),
        "gate_weight": gaussian(keys[4], (D, FF), D ** -0.5, 0.09375, ((0, 32), (1, 16))),
        "up_weight": gaussian(keys[5], (D, FF), D ** -0.5, 0.09375, ((0, 32), (1, 16))),
        "down_weight": gaussian(keys[6], (FF, D), FF ** -0.5, 0.0625, ((0, 16), (1, 32))),
        "norm_gain": jnp.clip(1.0 + 0.18 * jax.random.normal(keys[7], (D,), jnp.float32), 0.1, 1.9),
    }


def reference(tokens_in, grad_out, gate_pre, up_pre, gate_weight, up_weight, down_weight, norm_gain):
    gate_value = gate_pre.astype(jnp.float32)
    up_value = up_pre.astype(jnp.float32)
    gate_sigmoid = jax.nn.sigmoid(gate_value)
    gate_silu = gate_value * gate_sigmoid
    act = (gate_silu * up_value).astype(jnp.bfloat16)
    grad_act = jnp.dot(grad_out, down_weight.T, preferred_element_type=jnp.float32)
    grad_gate = (grad_act * up_value * gate_sigmoid * (1.0 + gate_value * (1.0 - gate_sigmoid))).astype(jnp.bfloat16)
    grad_up = (grad_act * gate_silu).astype(jnp.bfloat16)
    down_grad = jnp.dot(act.T, grad_out, preferred_element_type=jnp.float32).astype(jnp.bfloat16)
    width = FF // N_TENSOR

    def add_shard(total, index):
        start = index * width
        gate_cols = lax.dynamic_slice_in_dim(grad_gate, start, width, 1)
        up_cols = lax.dynamic_slice_in_dim(grad_up, start, width, 1)
        gate_part = lax.dynamic_slice_in_dim(gate_weight, start, width, 1)
        up_part = lax.dynamic_slice_in_dim(up_weight, start, width, 1)
        part = jnp.dot(gate_cols, gate_part.T, preferred_element_type=jnp.float32)
        part = part + jnp.dot(up_cols, up_part.T, preferred_element_type=jnp.float32)
        return (total + lax.optimization_barrier(part.astype(jnp.bfloat16)).astype(jnp.float32), None)
    grad_norm, unused_two = lax.scan(add_shard, jnp.zeros((TOKENS, D), jnp.float32), jnp.arange(N_TENSOR, dtype=jnp.int32))
    inputs = tokens_in.astype(jnp.float32)
    inv_rms = lax.rsqrt(lax.optimization_barrier(jnp.mean(inputs * inputs, axis=1, keepdims=True)) + 1e-05)
    normed = inputs * inv_rms
    gain_grad = lax.optimization_barrier(jnp.sum(grad_norm * normed, axis=0))
    scaled = grad_norm * norm_gain
    inner = lax.optimization_barrier(jnp.mean(scaled * normed, axis=1, keepdims=True))
    input_grad = (grad_out.astype(jnp.float32) + inv_rms * (scaled - normed * inner)).astype(jnp.bfloat16)
    return (input_grad, gain_grad, down_grad)
```

```python
import jax
import jax.numpy as jnp
from jax import lax
from jax.sharding import Mesh
from jax.sharding import PartitionSpec as P

Z = "dp_0"
YH = "dp_1"
TENSOR = ("tensor_0", "tensor_1", "tensor_2")
DP = ("dp_0", "dp_1")
DP_TENSOR = ("dp_0", "dp_1", "tensor_0", "tensor_1", "tensor_2")


def nt(a, b):
    return lax.dot_general(a, b, (((1,), (1,)), ((), ())), preferred_element_type=jnp.float32)


def tn(a, b):
    return lax.dot_general(a, b, (((0,), (0,)), ((), ())), preferred_element_type=jnp.float32)


def swap(x, axis):
    return lax.all_to_all(x, axis, split_axis=0, concat_axis=0, tiled=True)


def per_device(
    tokens_in, grad_out, gate_pre, up_pre, gate_weight, up_weight, down_weight, norm_gain
):
    mine = swap(grad_out.reshape(8, 8, 4, 128).transpose(2, 0, 1, 3), YH)
    rows = lax.all_gather(mine.reshape(32, 1024), TENSOR, axis=0, tiled=True)
    rows = rows.reshape(16, 4, 8, 1024).transpose(1, 0, 2, 3).reshape(512, 1024)
    down = lax.all_gather(down_weight, Z, axis=1, tiled=True)
    gate_w = lax.all_gather(gate_weight, Z, axis=0, tiled=True)
    up_w = lax.all_gather(up_weight, Z, axis=0, tiled=True)
    gate = lax.all_gather(gate_pre, YH, axis=0, tiled=True).astype(jnp.float32)
    up = lax.all_gather(up_pre, YH, axis=0, tiled=True).astype(jnp.float32)
    sig = jax.nn.sigmoid(gate)
    silu = gate * sig
    act = (silu * up).astype(jnp.bfloat16)
    part = nt(rows, down).astype(jnp.bfloat16).reshape(4, 128, 448)
    grad_act = swap(part, YH).astype(jnp.float32).sum(axis=0).astype(jnp.bfloat16)
    grad_act = lax.all_gather(grad_act, YH, axis=0, tiled=True).astype(jnp.float32)
    grad_gate = (grad_act * up * sig * (1.0 + gate * (1.0 - sig))).astype(jnp.bfloat16)
    grad_up = (grad_act * silu).astype(jnp.bfloat16)
    norm = (nt(grad_gate, gate_w) + nt(grad_up, up_w)).astype(jnp.bfloat16)
    norm = norm.reshape(4, 16, 8, 1024).transpose(1, 0, 2, 3)
    norm = swap(norm, TENSOR).astype(jnp.float32).sum(axis=0)
    norm = swap(norm, YH).reshape(4, 8, 8, 128)
    grad_norm = norm.transpose(1, 2, 0, 3).reshape(8, 4096)
    total = tn(act, rows).astype(jnp.bfloat16).reshape(448, 8, 128).transpose(1, 0, 2)
    down_grad = swap(total, Z).astype(jnp.float32).sum(axis=0).astype(jnp.bfloat16)

    inputs = tokens_in.astype(jnp.float32)
    inv_rms = lax.rsqrt(jnp.mean(inputs * inputs, axis=1, keepdims=True) + 1e-05)
    normed = inputs * inv_rms
    gain_grad = lax.psum(jnp.sum(grad_norm * normed, axis=0), DP_TENSOR)
    scaled = grad_norm * norm_gain
    inner = jnp.mean(scaled * normed, axis=1, keepdims=True)
    input_grad = (grad_out.astype(jnp.float32) + inv_rms * (scaled - normed * inner)).astype(
        jnp.bfloat16
    )
    return (input_grad, gain_grad, down_grad)


def solution(mesh):
    finer = Mesh(
        mesh.devices.reshape(8, 4, 4, 2, 2), ("dp_0", "dp_1", "tensor_0", "tensor_1", "tensor_2")
    )
    return jax.shard_map(
        per_device,
        mesh=finer,
        in_specs=(
            P(DP_TENSOR, None),
            P(DP_TENSOR, None),
            P(DP, TENSOR),
            P(DP, TENSOR),
            P(DP, TENSOR),
            P(DP, TENSOR),
            P(TENSOR, DP),
            P(),
        ),
        out_specs=(P(DP_TENSOR, None), P(), P(TENSOR, DP)),
        check_vma=False,
    )
```

```python
import jax
import jax.numpy as jnp
from jax import lax
from jax.experimental import pallas as pl
from jax.experimental.pallas import tpu as pltpu
from jax.sharding import Mesh
from jax.sharding import PartitionSpec as P

AXES = ("dp_0", "dp_1", "tensor_0", "tensor_1", "tensor_2")
Z, YH, X, YL, C = AXES
TENSOR = AXES[2:]
DP = AXES[:2]
BF = jnp.bfloat16
F32 = jnp.float32
MESH = pl.DeviceIdType.MESH
NZ, NY, NX = 8, 4, 4
N_SEND = 160


def dot(a, b, ca, cb):
    return lax.dot_general(a, b, (((ca,), (cb,)), ((), ())), preferred_element_type=F32)


def kernel(
    tok, gout, gate, up, gw, uw, dw, gain,
    igrad, ggrad, dgrad,
    w, gu, a, st, fac, act, sa, ra, own, ga, pn, rn, qn, rq, fs, fn, ds_, rd, gacc,
    g1, g2, g3, g4, irms,
    ssem, wsem, gsem, s1sem, ylsem, xsem, csem, rasem, gasem, rnsem, rqsem, fnsem, rdsem,
    g1sem, g2sem, g3sem, g4sem,
):
    z, k, x = lax.axis_index(Z), lax.axis_index(YH), lax.axis_index(X)
    yl, c = lax.axis_index(YL), lax.axis_index(C)
    t = x * 4 + yl * 2 + c
    sends = []

    def send(src, dst, dev, rsem):
        cp = pltpu.make_async_remote_copy(
            src_ref=src, dst_ref=dst, send_sem=ssem.at[len(sends)], recv_sem=rsem,
            device_id=dev, device_id_type=MESH,
        )
        cp.start()
        sends.append(cp)

    def arrived(ref, rsem):
        pltpu.make_async_copy(ref, ref, rsem).wait()

    def zz(d):
        return lax.rem(z + d + NZ, NZ)

    def yy(d):
        return lax.rem(k + d + NY, NY)

    def xx(d):
        return lax.rem(x + d, NX)

    xc = [(d, e) for d in range(NX) for e in range(2) if d or e]

    def xc_dev(d, e):
        return {X: xx(d), C: lax.rem(c + e, 2)}

    peers = [{Z: zz(d)} for d in range(1, NZ)] + [{YH: yy(d)} for d in range(1, NY)]
    peers += [xc_dev(d, e) for d, e in xc] + [{YL: 1 - yl}]
    barrier = pltpu.get_barrier_semaphore()
    for p in peers:
        pl.semaphore_signal(barrier, inc=1, device_id=p, device_id_type=MESH)

    for q in range(NY):
        for i in range(NZ):
            col = (i * NY + q) * 128
            st[0, q, :, i * 128:(i + 1) * 128] = gout[:, col:col + 128]
    a[0, k, t] = st[0, k]
    pl.semaphore_wait(barrier, len(peers))

    w_in = (dw, gw, uw)
    gu_in = (gate, up)

    def ring_first(src, buf, me, left, right, sem):
        send(src, buf.at[me], right, sem.at[0, 0])
        send(src, buf.at[me], left, sem.at[1, 0])

    def ring_next(buf, at, s, n, left, right, sem):
        for way, dev in ((0, right), (1, left)):
            slot = buf.at[at(-s if way == 0 else s)]
            arrived(slot, sem.at[way, s - 1])
            if s + 1 < n // 2:
                send(slot, slot, dev, sem.at[way, s])
            else:
                half = slot.at[pl.ds(224 * way, 224)]
                send(half, half, dev, sem.at[way, s])

    def ring_last(buf, at, n, sem):
        slot = buf.at[at(n // 2)]
        for way in range(2):
            arrived(slot.at[pl.ds(224 * way, 224)], sem.at[way, n // 2 - 1])

    zl, zr, yl_, yr_ = {Z: zz(-1)}, {Z: zz(1)}, {YH: yy(-1)}, {YH: yy(1)}

    def w_first(i):
        ring_first(w_in[i], w.at[i], z, zl, zr, wsem.at[i])

    def w_next(i, s):
        ring_next(w.at[i], zz, s, NZ, zl, zr, wsem.at[i])

    def gu_first(i):
        ring_first(gu_in[i], gu.at[i], k, yl_, yr_, gsem.at[i])

    def s1_send(i):
        for d in (2, 1, 3):
            send(st.at[i, yy(d)], a.at[i, k, t], {YH: yy(d)}, s1sem.at[i, d])

    def s1_wait(i):
        for d in (1, 3, 2):
            arrived(a.at[i, yy(-d), t], s1sem.at[i, d])

    def unit(i, t_):
        return a.at[i, :, t_]

    core = {C: 1 - c}
    t_yl = x * 4 + (1 - yl) * 2 + c

    def unit_send(i, j, tj):
        for d in (2, 1, 3):
            send(unit(i, tj), unit(i, tj), {X: xx(d)}, xsem.at[i, j, d])
        send(unit(i, tj), unit(i, tj), core, csem.at[i, 0, j])

    def t_of(d, j):
        return lax.rem(x + NX - d, NX) * 4 + (yl if j == 0 else 1 - yl) * 2 + c

    def unit_x(i, j):
        for d in (1, 3, 2):
            td = t_of(d, j)
            arrived(unit(i, td), xsem.at[i, j, d])
            send(unit(i, td), unit(i, td), core, csem.at[i, d, j])

    def unit_core(i):
        for j in range(2):
            for d in range(NX):
                tc = lax.rem(x + NX - d, NX) * 4 + (yl if j == 0 else 1 - yl) * 2 + 1 - c
                arrived(unit(i, tc), csem.at[i, d, j])

    w_first(0)
    s1_send(0)
    gu_first(0)
    w_first(1)
    gu_first(1)

    tf = tok[...].astype(F32)
    inv = lax.rsqrt(jnp.mean(tf * tf, axis=1, keepdims=True) + 1e-05)
    irms[...] = jnp.broadcast_to(inv, (8, 128))
    for q in range(NY):
        for i in range(NZ):
            col = (i * NY + q) * 128
            st[1, q, :, i * 128:(i + 1) * 128] = (tf[:, col:col + 128] * inv).astype(BF)
    a[1, k, t] = st[1, k]
    for i in range(3):
        w[i, z] = w_in[i][...]
    for i in range(2):
        gu[i, k] = gu_in[i][...]

    s1_wait(0)
    send(unit(0, t), unit(0, t), {YL: 1 - yl}, ylsem.at[0])
    unit_send(0, 0, t)
    w_next(0, 1)
    w_first(2)
    arrived(unit(0, t_yl), ylsem.at[0])
    unit_send(0, 1, t_yl)
    w_next(1, 1)
    w_next(0, 2)
    for i in range(2):
        ring_next(gu.at[i], yy, 1, NY, yl_, yr_, gsem.at[i])
    s1_send(1)
    unit_x(0, 0)
    w_next(2, 1)
    w_next(0, 3)
    unit_x(0, 1)
    w_next(1, 2)
    unit_core(0)
    ring_last(w.at[0], zz, NZ, wsem.at[0])

    down = jnp.concatenate([w[0, i] for i in range(NZ)], axis=1)
    for d in (2, 1, 3, 0):
        rows = a.at[0, yy(d)].reshape(128, 1024)[...]
        part = dot(down, rows, 1, 1)
        if d:
            sa[d] = part.astype(BF)
            send(sa.at[d], ra.at[d], {YH: yy(d)}, rasem.at[d])
        else:
            own[...] = part

    for i in range(2):
        ring_last(gu.at[i], yy, NY, gsem.at[i])
    for j in range(NY):
        gv = gu[0, j].astype(F32)
        uv = gu[1, j].astype(F32)
        sg = jax.nn.sigmoid(gv)
        sv = gv * sg
        fac[0, j] = uv * sg * (1.0 + gv * (1.0 - sg))
        fac[1, j] = sv
        act[j] = (sv * uv).astype(BF)

    w_next(2, 2)
    w_next(1, 3)
    w_next(2, 3)
    s1_wait(1)
    send(unit(1, t), unit(1, t), {YL: 1 - yl}, ylsem.at[1])
    unit_send(1, 0, t)

    for d in (1, 3, 2):
        arrived(ra.at[d], rasem.at[d])
    total = own[...] + ra[1].astype(F32) + ra[2].astype(F32) + ra[3].astype(F32)
    ga[k] = total.astype(BF)
    for d in (2, 1, 3):
        send(ga.at[k], ga.at[k], {YH: yy(d)}, gasem.at[d])

    arrived(unit(1, t_yl), ylsem.at[1])
    unit_send(1, 1, t_yl)
    for i in (1, 2):
        ring_last(w.at[i], zz, NZ, wsem.at[i])

    acts = jnp.concatenate([act[j] for j in range(NY)], axis=1)
    rows_all = a.at[0].reshape(512, 1024)
    for i in range(NZ // 2):
        pair = dot(acts, rows_all[:, i * 256:(i + 1) * 256], 1, 0)
        ds_[2 * i] = pair[:, :128].astype(BF)
        ds_[2 * i + 1] = pair[:, 128:].astype(BF)
    for d in (4, 3, 5, 2, 6, 1, 7):
        send(ds_.at[zz(d)], rd.at[d], {Z: zz(d)}, rdsem.at[d])

    unit_x(1, 0)
    unit_x(1, 1)
    unit_core(1)

    gacc[...] = jnp.zeros((8, 1024), F32)
    for d in (0, 1, 3, 2):
        j = yy(-d)
        if d:
            arrived(ga.at[j], gasem.at[d])
        gj = ga[j].astype(F32)
        both = jnp.concatenate([(gj * fac[0, j]).astype(BF), (gj * fac[1, j]).astype(BF)], axis=0)
        for i in range(NZ // 2):
            cols = jnp.concatenate(
                [
                    jnp.concatenate([w[1, 2 * i], w[2, 2 * i]], axis=0),
                    jnp.concatenate([w[1, 2 * i + 1], w[2, 2 * i + 1]], axis=0),
                ],
                axis=1,
            )
            part = dot(both, cols, 0, 0)
            lanes = slice(i * 256, (i + 1) * 256)
            add = gacc[:, lanes]
            for q in range(16):
                piece = part[q * 8:(q + 1) * 8]
                pn[d, q // 4, (q // 2) % 2, q % 2, :, lanes] = piece.astype(BF)
                add = add + piece * a[1, j, q, :, lanes].astype(F32)
            gacc[:, lanes] = add
        for e, f in sorted(xc, key=lambda v: -min(v[0], 4 - v[0])):
            send(
                pn.at[d, xx(e), :, lax.rem(c + f, 2)], rn.at[d, e * 2 + f],
                xc_dev(e, f), rnsem.at[d, e * 2 + f],
            )

    for i in range(NZ):
        g1[x * 2 + c, i:i + 1, :] = jnp.sum(
            gacc[:, i * 128:(i + 1) * 128], axis=0, keepdims=True
        )
    for e, f in xc:
        send(g1.at[x * 2 + c], g1.at[x * 2 + c], xc_dev(e, f), g1sem.at[e * 2 + f])

    def norm_first(d):
        for e, f in xc:
            arrived(rn.at[d, e * 2 + f], rnsem.at[d, e * 2 + f])
        for_peer = pn[d, x, 1 - yl, c].astype(F32)
        for e, f in xc:
            for_peer = for_peer + rn[d, e * 2 + f, 1 - yl].astype(F32)
        qn[d] = for_peer.astype(BF)
        send(qn.at[d], rq.at[d], {YL: 1 - yl}, rqsem.at[d])

    def norm_second(d):
        mine = pn[d, x, yl, c].astype(F32)
        for e, f in xc:
            mine = mine + rn[d, e * 2 + f, yl].astype(F32)
        arrived(rq.at[d], rqsem.at[d])
        mine = mine + rq[d].astype(F32)
        if d:
            fs[d] = mine
            send(fs.at[d], fn.at[k], {YH: yy(-d)}, fnsem.at[d])
        else:
            fn[k] = mine

    norm_first(1)
    norm_first(3)
    norm_second(1)
    norm_second(3)
    norm_first(2)
    norm_first(0)
    for e, f in xc:
        arrived(g1.at[lax.rem(x + NX - e, NX) * 2 + lax.rem(c + f, 2)], g1sem.at[e * 2 + f])
    g2[yl] = jnp.sum(g1[...], axis=0)
    send(g2.at[yl], g2.at[yl], {YL: 1 - yl}, g2sem.at[0])
    norm_second(2)
    norm_second(0)
    arrived(g2.at[1 - yl], g2sem.at[0])
    g3[z] = g2[0] + g2[1]
    for d in (4, 3, 5, 2, 6, 1, 7):
        send(g3.at[z], g3.at[z], {Z: zz(d)}, g3sem.at[d])

    for d in range(1, NZ):
        arrived(rd.at[d], rdsem.at[d])
    dsum = ds_[z].astype(F32)
    for d in range(1, NZ):
        dsum = dsum + rd[d].astype(F32)
    dgrad[...] = dsum.astype(BF)

    for d in range(1, NZ):
        arrived(g3.at[zz(-d)], g3sem.at[d])
    g4[k] = jnp.sum(g3[...], axis=0)
    for d in (2, 1, 3):
        send(g4.at[k], g4.at[k], {YH: yy(d)}, g4sem.at[d])

    for d in (1, 3, 2):
        arrived(fn.at[yy(d)], fnsem.at[d])
    inv = irms[...]
    inner = jnp.zeros((8, 128), F32)
    for i in range(NZ):
        for q in range(NY):
            b = i * NY + q
            normed = tok[:, b * 128:(b + 1) * 128].astype(F32) * inv
            inner = inner + fn[q, :, i * 128:(i + 1) * 128] * gain[b:b + 1, :] * normed
    inner = jnp.sum(inner, axis=1, keepdims=True) * (1.0 / 4096)
    for i in range(NZ):
        for q in range(NY):
            b = i * NY + q
            cols = slice(b * 128, (b + 1) * 128)
            normed = tok[:, cols].astype(F32) * inv
            scaled = fn[q, :, i * 128:(i + 1) * 128] * gain[b:b + 1, :]
            igrad[:, cols] = (
                gout[:, cols].astype(F32) + inv * (scaled - normed * inner)
            ).astype(BF)

    for d in range(1, NY):
        arrived(g4.at[yy(-d)], g4sem.at[d])
    for i in range(NZ):
        for q in range(NY):
            b = i * NY + q
            ggrad[b:b + 1, :] = g4[q, i:i + 1, :]
    for cp in sends:
        cp.wait_send()


def per_device(
    tokens_in, grad_out, gate_pre, up_pre, gate_weight, up_weight, down_weight, norm_gain
):
    vm = pltpu.VMEM
    dma = pltpu.SemaphoreType.DMA
    scratch = [
        vm((3, NZ, 448, 128), BF),
        vm((2, NY, 448, 128), BF),
        vm((2, NY, 16, 8, 1024), BF),
        vm((2, NY, 8, 1024), BF),
        vm((2, NY, 448, 128), F32),
        vm((NY, 448, 128), BF),
        vm((NY, 448, 128), BF),
        vm((NY, 448, 128), BF),
        vm((448, 128), F32),
        vm((NY, 448, 128), BF),
        vm((NY, NX, 2, 2, 8, 1024), BF),
        vm((NY, 8, 2, 8, 1024), BF),
        vm((NY, 8, 1024), BF),
        vm((NY, 8, 1024), BF),
        vm((NY, 8, 1024), F32),
        vm((NY, 8, 1024), F32),
        vm((NZ, 448, 128), BF),
        vm((NZ, 448, 128), BF),
        vm((8, 1024), F32),
        vm((8, 8, 128), F32),
        vm((2, 8, 128), F32),
        vm((NZ, 8, 128), F32),
        vm((NY, 8, 128), F32),
        vm((8, 128), F32),
        dma((N_SEND,)),
        dma((3, 2, 4)),
        dma((2, 2, 2)),
        dma((2, 4)),
        dma((2,)),
        dma((2, 2, 4)),
        dma((2, 4, 2)),
        dma((4,)),
        dma((4,)),
        dma((4, 8)),
        dma((4,)),
        dma((4,)),
        dma((8,)),
        dma((8,)),
        dma((1,)),
        dma((8,)),
        dma((4,)),
    ]
    spec = pl.BlockSpec(memory_space=pltpu.VMEM)
    igrad, ggrad, dgrad = pl.pallas_call(
        kernel,
        out_shape=(
            jax.ShapeDtypeStruct((8, 4096), BF),
            jax.ShapeDtypeStruct((32, 128), F32),
            jax.ShapeDtypeStruct((448, 128), BF),
        ),
        in_specs=[spec] * 8,
        out_specs=(spec,) * 3,
        scratch_shapes=scratch,
        compiler_params=pltpu.CompilerParams(
            collective_id=0, has_side_effects=True, vmem_limit_bytes=60 * 1024 * 1024
        ),
    )(
        tokens_in, grad_out, gate_pre.T, up_pre.T, gate_weight.T, up_weight.T, down_weight,
        norm_gain.reshape(32, 128),
    )
    return igrad, ggrad.reshape(4096), dgrad


def solution(mesh):
    finer = Mesh(mesh.devices.reshape(NZ, NY, NX, 2, 2), AXES)
    return jax.shard_map(
        per_device,
        mesh=finer,
        in_specs=(
            P(AXES, None),
            P(AXES, None),
            P(DP, TENSOR),
            P(DP, TENSOR),
            P(DP, TENSOR),
            P(DP, TENSOR),
            P(TENSOR, DP),
            P(),
        ),
        out_specs=(P(AXES, None), P(), P(TENSOR, DP)),
        check_vma=False,
    )
```

```python
import jax
import jax.numpy as jnp
from jax import lax
from jax.experimental import pallas as pl
from jax.experimental.pallas import tpu as pltpu
from jax.sharding import Mesh
from jax.sharding import PartitionSpec as P

AXES = ("dp_0", "dp_1", "tensor_0", "tensor_1", "tensor_2")
Z, YH, X, YL, C = AXES
TENSOR = AXES[2:]
DP = AXES[:2]
BF = jnp.bfloat16
F32 = jnp.float32
MESH = pl.DeviceIdType.MESH
NZ, NY, NX = 8, 4, 4
N_SEND = 200


def dot(a, b, ca, cb):
    return lax.dot_general(a, b, (((ca,), (cb,)), ((), ())), preferred_element_type=F32)


def kernel(
    tok_h, gout_h, gate_h, up_h, gw_h, uw_h, dw_h, gain_h,
    igrad, ggrad, dgrad,
    tok, gout, gain,
    w, gu, a, st, fac, act, sa, ra, rb, part, ga, pn, rn, qn, rq, fs, fn, ds_, rd, gacc,
    g1, g2, g3, g4, irms,
    lsem, ssem, wsem, gsem, s1sem, xsem, csem, rasem, rbsem, gasem, rnsem, rqsem, fnsem, rdsem,
    g1sem, g2sem, g3sem, g4sem,
):
    z, k, x = lax.axis_index(Z), lax.axis_index(YH), lax.axis_index(X)
    yl, c = lax.axis_index(YL), lax.axis_index(C)
    sends = []

    def send(src, dst, dev, rsem):
        cp = pltpu.make_async_remote_copy(
            src_ref=src, dst_ref=dst, send_sem=ssem.at[len(sends)], recv_sem=rsem,
            device_id=dev, device_id_type=MESH,
        )
        cp.start()
        sends.append(cp)

    def arrived(ref, rsem):
        pltpu.make_async_copy(ref, ref, rsem).wait()

    def zz(d):
        return lax.rem(z + d + NZ, NZ)

    def yy(d):
        return lax.rem(k + d + NY, NY)

    def xx(d):
        return lax.rem(x + d + NX, NX)

    def ee(v, e):
        return lax.rem(v + e, 2)

    xc = [(d, e) for d in (2, 1, 3, 0) for e in range(2) if d or e]
    ys = [(d, e) for d in (2, 1, 3, 0) for e in (1, 0) if d or e]
    zs = (4, 3, 5, 2, 6, 1, 7)

    def xc_dev(d, e):
        return {X: xx(d), C: ee(c, e)}

    def ys_dev(d, e):
        return {YH: yy(d), YL: ee(yl, e)}

    peers = [{Z: zz(d)} for d in zs]
    peers += [ys_dev(d, e) for d, e in ys] + [xc_dev(d, e) for d, e in xc]
    barrier = pltpu.get_barrier_semaphore()
    for p in peers:
        pl.semaphore_signal(barrier, inc=1, device_id=p, device_id_type=MESH)

    loads = [
        (gout_h, gout), (tok_h, tok), (dw_h, w.at[0, z]), (gate_h, gu.at[0, k]),
        (up_h, gu.at[1, k]), (gw_h, w.at[1, z]), (uw_h, w.at[2, z]), (gain_h, gain),
    ]
    loads = [pltpu.make_async_copy(s, d, lsem.at[i]) for i, (s, d) in enumerate(loads)]
    for cp in loads:
        cp.start()

    loads[0].wait()
    for q in range(NY):
        for i in range(NZ):
            col = (i * NY + q) * 128
            st[0, q, :, i * 128:(i + 1) * 128] = gout[:, col:col + 128]
    a[0, k, x, yl, c] = st[0, k]
    loads[1].wait()
    tf = tok[...].astype(F32)
    inv = lax.rsqrt(jnp.mean(tf * tf, axis=1, keepdims=True) + 1e-05)
    irms[...] = jnp.broadcast_to(inv, (8, 128))
    for q in range(NY):
        for i in range(NZ):
            col = (i * NY + q) * 128
            st[1, q, :, i * 128:(i + 1) * 128] = (tf[:, col:col + 128] * inv).astype(BF)
    a[1, k, x, yl, c] = st[1, k]
    for cp in loads[2:]:
        cp.wait()
    pl.semaphore_wait(barrier, len(peers))

    def half(ref, h):
        return ref.at[pl.ds(224 * h, 224)]

    class Ring:
        def __init__(self, buf, at, me, n, left, right, sem):
            self.buf, self.at, self.me, self.n, self.sem = buf, at, me, n, sem
            self.devs = (right, left)

        def put(self, slot, way, step, h):
            p = half(self.buf.at[slot], h)
            send(p, p, self.devs[way], self.sem.at[way, step, h])

        def first(self):
            for i in range(2):
                for way in range(2):
                    self.put(self.me, way, 0, i ^ way)

        def got(self, s, way, h):
            slot = self.at(-s if way == 0 else s)
            arrived(half(self.buf.at[slot], h), self.sem.at[way, s - 1, h])
            return slot

        def nxt(self, s):
            for i in range(2):
                for way in range(2):
                    slot = self.got(s, way, i ^ way)
                    if s + 1 < self.n // 2 or i == 0:
                        self.put(slot, way, s, i ^ way)

        def last(self):
            for way in range(2):
                self.got(self.n // 2, way, way)

    zl, zr, kl, kr = {Z: zz(-1)}, {Z: zz(1)}, {YH: yy(-1)}, {YH: yy(1)}
    dwr, gwr, uwr = [Ring(w.at[i], zz, z, NZ, zl, zr, wsem.at[i]) for i in range(3)]
    gater, upr = [Ring(gu.at[i], yy, k, NY, kl, kr, gsem.at[i]) for i in range(2)]
    gar = Ring(ga, yy, k, NY, kl, kr, gasem)
    core = {C: 1 - c}

    def s1_send(i):
        for d, e in ys:
            send(st.at[i, yy(d)], a.at[i, k, x, yl, c], ys_dev(d, e), s1sem.at[i, d * 2 + e])

    def s1_wait(i):
        for d, e in reversed(ys):
            arrived(a.at[i, yy(-d), x, ee(yl, e), c], s1sem.at[i, d * 2 + e])

    def unit(i, xs, cs):
        return a.at[i, :, xs, :, cs]

    def x_send(i):
        for d in (2, 1, 3):
            send(unit(i, x, c), unit(i, x, c), {X: xx(d)}, xsem.at[i, d])
        send(unit(i, x, c), unit(i, x, c), core, csem.at[i, 0])

    def x_wait(i):
        for d in (1, 3, 2):
            u = unit(i, xx(-d), c)
            arrived(u, xsem.at[i, d])
            send(u, u, core, csem.at[i, d])

    def core_wait(i):
        for d in (0, 1, 3, 2):
            arrived(unit(i, xx(-d), 1 - c), csem.at[i, d])

    dwr.first()
    s1_send(0)
    gater.first()
    dwr.nxt(1)
    s1_wait(0)
    x_send(0)
    dwr.nxt(2)
    dwr.nxt(3)
    gwr.first()
    gater.nxt(1)
    upr.first()
    uwr.first()
    x_wait(0)
    dwr.last()
    gwr.nxt(1)
    core_wait(0)

    down = jnp.concatenate([w[0, i] for i in range(NZ)], axis=1)

    def partial(d):
        return dot(down, a.at[0, yy(d)].reshape(128, 1024)[...], 1, 1)

    sa[1] = partial(2).astype(BF)
    send(half(sa.at[1], 0), rb.at[0], kr, rbsem.at[0])
    send(half(sa.at[1], 1), rb.at[1], kl, rbsem.at[1])
    for n, (d, dev, h) in enumerate(((1, kr, 1), (3, kl, 0))):
        rows = slice(224 * h, 224 * h + 224)
        part[n] = partial(d)
        sa[2 * n, rows] = part[n, rows].astype(BF)
        send(half(sa.at[2 * n], h), half(ra.at[n], h), dev, rasem.at[n, h])
    part[2] = partial(0)

    uwr.nxt(1)
    upr.nxt(1)
    gwr.nxt(2)

    for n, (dev, h) in enumerate(((kr, 0), (kl, 1))):
        rows = slice(224 * h, 224 * h + 224)
        arrived(rb.at[n], rbsem.at[n])
        sa[2 * n, rows] = (part[n, rows] + rb[n].astype(F32)).astype(BF)
        send(half(sa.at[2 * n], h), half(ra.at[n], h), dev, rasem.at[n, h])
    s1_send(1)

    uwr.nxt(2)

    gater.last()
    upr.last()
    for j in range(NY):
        gv = gu[0, j].astype(F32)
        uv = gu[1, j].astype(F32)
        sg = jax.nn.sigmoid(gv)
        sv = gv * sg
        fac[0, j] = uv * sg * (1.0 + gv * (1.0 - sg))
        fac[1, j] = sv
        act[j] = (sv * uv).astype(BF)
    gwr.nxt(3)

    for n in range(2):
        for h in range(2):
            arrived(half(ra.at[n], h), rasem.at[n, h])
    ga[k] = (part[2] + ra[0].astype(F32) + ra[1].astype(F32)).astype(BF)
    gar.first()

    uwr.nxt(3)
    s1_wait(1)
    x_send(1)
    gwr.last()
    uwr.last()

    def norm_part(d):
        j = yy(-d)
        gj = ga[j].astype(F32)
        both = jnp.concatenate([(gj * fac[0, j]).astype(BF), (gj * fac[1, j]).astype(BF)], axis=0)
        for i in range(NZ // 2):
            cols = jnp.concatenate(
                [
                    jnp.concatenate([w[1, 2 * i], w[2, 2 * i]], axis=0),
                    jnp.concatenate([w[1, 2 * i + 1], w[2, 2 * i + 1]], axis=0),
                ],
                axis=1,
            )
            block = dot(both, cols, 0, 0)
            lanes = slice(i * 256, (i + 1) * 256)
            for q in range(16):
                pn[d, q // 4, (q // 2) % 2, q % 2, :, lanes] = block[q * 8:(q + 1) * 8].astype(BF)
        for e, f in xc:
            send(
                pn.at[d, xx(e), :, ee(c, f)], rn.at[d, e * 2 + f],
                xc_dev(e, f), rnsem.at[d, e * 2 + f],
            )

    def norm_first(d):
        for e, f in reversed(xc):
            arrived(rn.at[d, e * 2 + f], rnsem.at[d, e * 2 + f])
        for_peer = pn[d, x, 1 - yl, c].astype(F32)
        for e, f in xc:
            for_peer = for_peer + rn[d, e * 2 + f, 1 - yl].astype(F32)
        qn[d] = for_peer.astype(BF)
        send(qn.at[d], rq.at[d], {YL: 1 - yl}, rqsem.at[d])

    def norm_second(d):
        mine = pn[d, x, yl, c].astype(F32)
        for e, f in xc:
            mine = mine + rn[d, e * 2 + f, yl].astype(F32)
        arrived(rq.at[d], rqsem.at[d])
        mine = mine + rq[d].astype(F32)
        if d:
            fs[d] = mine
            send(fs.at[d], fn.at[k], {YH: yy(-d)}, fnsem.at[d])
        else:
            fn[k] = mine

    norm_part(0)

    acts = jnp.concatenate([act[j] for j in range(NY)], axis=1)
    rows_all = a.at[0].reshape(512, 1024)
    for i in range(NZ // 2):
        pair = dot(acts, rows_all[:, i * 256:(i + 1) * 256], 1, 0)
        ds_[2 * i] = pair[:, :128].astype(BF)
        ds_[2 * i + 1] = pair[:, 128:].astype(BF)
    for d in zs:
        send(ds_.at[zz(d)], rd.at[d], {Z: zz(d)}, rdsem.at[d])

    gar.nxt(1)
    norm_part(1)
    norm_part(3)
    x_wait(1)
    norm_first(0)
    gar.last()
    norm_part(2)

    core_wait(1)
    add = jnp.zeros((8, 1024), F32)
    for d in range(NY):
        for q in range(16):
            at = (q // 4, (q // 2) % 2, q % 2)
            add = add + pn[(d,) + at].astype(F32) * a[(1, yy(-d)) + at].astype(F32)
    for i in range(NZ):
        g1[x * 2 + c, i:i + 1, :] = jnp.sum(add[:, i * 128:(i + 1) * 128], axis=0, keepdims=True)
    for e, f in xc:
        send(g1.at[x * 2 + c], g1.at[x * 2 + c], xc_dev(e, f), g1sem.at[e * 2 + f])

    norm_second(0)
    norm_first(1)
    norm_first(3)
    for e, f in reversed(xc):
        arrived(g1.at[xx(-e) * 2 + ee(c, f)], g1sem.at[e * 2 + f])
    g2[yl] = jnp.sum(g1[...], axis=0)
    send(g2.at[yl], g2.at[yl], {YL: 1 - yl}, g2sem.at[0])
    norm_second(1)
    norm_second(3)
    norm_first(2)
    arrived(g2.at[1 - yl], g2sem.at[0])
    g3[z] = g2[0] + g2[1]
    for d in zs:
        send(g3.at[z], g3.at[z], {Z: zz(d)}, g3sem.at[d])
    norm_second(2)

    for d in reversed(zs):
        arrived(rd.at[d], rdsem.at[d])
    dsum = ds_[z].astype(F32)
    for d in range(1, NZ):
        dsum = dsum + rd[d].astype(F32)
    dgrad[...] = dsum.astype(BF)

    for d in reversed(zs):
        arrived(g3.at[zz(-d)], g3sem.at[d])
    g4[k] = jnp.sum(g3[...], axis=0)
    for d in (2, 1, 3):
        send(g4.at[k], g4.at[k], {YH: yy(d)}, g4sem.at[d])

    for d in (1, 3, 2):
        arrived(fn.at[yy(d)], fnsem.at[d])
    inv = irms[...]
    inner = jnp.zeros((8, 128), F32)
    for i in range(NZ):
        for q in range(NY):
            b = i * NY + q
            normed = tok[:, b * 128:(b + 1) * 128].astype(F32) * inv
            inner = inner + fn[q, :, i * 128:(i + 1) * 128] * gain[b:b + 1, :] * normed
    inner = jnp.sum(inner, axis=1, keepdims=True) * (1.0 / 4096)
    for i in range(NZ):
        for q in range(NY):
            b = i * NY + q
            cols = slice(b * 128, (b + 1) * 128)
            normed = tok[:, cols].astype(F32) * inv
            scaled = fn[q, :, i * 128:(i + 1) * 128] * gain[b:b + 1, :]
            igrad[:, cols] = (
                gout[:, cols].astype(F32) + inv * (scaled - normed * inner)
            ).astype(BF)

    for d in range(1, NY):
        arrived(g4.at[yy(-d)], g4sem.at[d])
    for i in range(NZ):
        for q in range(NY):
            b = i * NY + q
            ggrad[b:b + 1, :] = g4[q, i:i + 1, :]
    for cp in sends:
        cp.wait_send()


def per_device(
    tokens_in, grad_out, gate_pre, up_pre, gate_weight, up_weight, down_weight, norm_gain
):
    vm = pltpu.VMEM
    dma = pltpu.SemaphoreType.DMA
    scratch = [
        vm((8, 4096), BF),
        vm((8, 4096), BF),
        vm((32, 128), F32),
        vm((3, NZ, 448, 128), BF),
        vm((2, NY, 448, 128), BF),
        vm((2, NY, NX, 2, 2, 8, 1024), BF),
        vm((2, NY, 8, 1024), BF),
        vm((2, NY, 448, 128), F32),
        vm((NY, 448, 128), BF),
        vm((3, 448, 128), BF),
        vm((2, 448, 128), BF),
        vm((2, 224, 128), BF),
        vm((3, 448, 128), F32),
        vm((NY, 448, 128), BF),
        vm((NY, NX, 2, 2, 8, 1024), BF),
        vm((NY, 8, 2, 8, 1024), BF),
        vm((NY, 8, 1024), BF),
        vm((NY, 8, 1024), BF),
        vm((NY, 8, 1024), F32),
        vm((NY, 8, 1024), F32),
        vm((NZ, 448, 128), BF),
        vm((NZ, 448, 128), BF),
        vm((8, 1024), F32),
        vm((8, 8, 128), F32),
        vm((2, 8, 128), F32),
        vm((NZ, 8, 128), F32),
        vm((NY, 8, 128), F32),
        vm((8, 128), F32),
        dma((8,)),
        dma((N_SEND,)),
        dma((3, 2, 4, 2)),
        dma((2, 2, 2, 2)),
        dma((2, 8)),
        dma((2, 4)),
        dma((2, 4)),
        dma((2, 2)),
        dma((2,)),
        dma((2, 2, 2)),
        dma((4, 8)),
        dma((4,)),
        dma((4,)),
        dma((8,)),
        dma((8,)),
        dma((1,)),
        dma((8,)),
        dma((4,)),
    ]
    spec = pl.BlockSpec(memory_space=pltpu.VMEM)
    hbm = pl.BlockSpec(memory_space=pl.ANY)
    igrad, ggrad, dgrad = pl.pallas_call(
        kernel,
        out_shape=(
            jax.ShapeDtypeStruct((8, 4096), BF),
            jax.ShapeDtypeStruct((32, 128), F32),
            jax.ShapeDtypeStruct((448, 128), BF),
        ),
        in_specs=[hbm] * 8,
        out_specs=(spec,) * 3,
        scratch_shapes=scratch,
        compiler_params=pltpu.CompilerParams(
            collective_id=0, has_side_effects=True, vmem_limit_bytes=60 * 1024 * 1024
        ),
    )(
        tokens_in, grad_out, gate_pre.T, up_pre.T, gate_weight.T, up_weight.T, down_weight,
        norm_gain.reshape(32, 128),
    )
    return igrad, ggrad.reshape(4096), dgrad


def solution(mesh):
    finer = Mesh(mesh.devices.reshape(NZ, NY, NX, 2, 2), AXES)
    return jax.shard_map(
        per_device,
        mesh=finer,
        in_specs=(
            P(AXES, None),
            P(AXES, None),
            P(DP, TENSOR),
            P(DP, TENSOR),
            P(DP, TENSOR),
            P(DP, TENSOR),
            P(TENSOR, DP),
            P(),
        ),
        out_specs=(P(AXES, None), P(), P(TENSOR, DP)),
        check_vma=False,
    )
```

```python
import jax
import jax.numpy as jnp
from jax import lax
from jax.experimental import pallas as pl
from jax.experimental.pallas import tpu as pltpu
from jax.sharding import Mesh
from jax.sharding import PartitionSpec as P

AXES = ("dp_0", "dp_1", "tensor_0", "tensor_1", "tensor_2")
Z, YH, X, YL, C = AXES
TENSOR = AXES[2:]
DP = AXES[:2]
BF = jnp.bfloat16
F32 = jnp.float32
MESH = pl.DeviceIdType.MESH
NZ, NY, NX = 8, 4, 4


def dot(a, b, ca, cb):
    return lax.dot_general(a, b, (((ca,), (cb,)), ((), ())), preferred_element_type=F32)


def kernel(
    tok_h, gout_h, gate_h, up_h, gw_h, uw_h, dw_h, gain_h,
    igrad, ggrad, dgrad,
    tok, gout, gain,
    w, gu, a, st, fac, act, sa, ra, rb, part, ga, pn, rc, sx, rx, fs, fn, gn, ds_, rd, gacc,
    g1, g3, g4, irms,
    lsem, ssem, wsem, gsem, s1sem, xsem, csem, rasem, rbsem, gasem, rcsem, rxsem, fnsem, rdsem,
    g1sem, g3sem, g4sem,
):
    z, k, x = lax.axis_index(Z), lax.axis_index(YH), lax.axis_index(X)
    yl, c = lax.axis_index(YL), lax.axis_index(C)
    sends = []

    def send(src, dst, dev, rsem, group):
        if group not in sends:
            sends.append(group)
        pltpu.make_async_remote_copy(
            src_ref=src, dst_ref=dst, send_sem=ssem.at[sends.index(group)], recv_sem=rsem,
            device_id=dev, device_id_type=MESH,
        ).start()

    def arrived(ref, rsem):
        pltpu.make_async_copy(ref, ref, rsem).wait()

    def units(n):
        return a.at[0].reshape(512, 1024).at[pl.ds(0, 8 * n)]

    def zz(d):
        return lax.rem(z + d + NZ, NZ)

    def yy(d):
        return lax.rem(k + d + NY, NY)

    def xx(d):
        return lax.rem(x + d + NX, NX)

    def ee(v, e):
        return lax.rem(v + e, 2)

    ys = [(d, e) for d in (2, 1, 3, 0) for e in (1, 0) if d or e]
    zs = (4, 3, 5, 2, 6, 1, 7)
    ts = [(d, e, f) for d in (2, 1, 3, 0) for e in (1, 0) for f in (1, 0) if d or e or f]

    def ts_dev(d, e, f):
        return {X: xx(d), YL: ee(yl, e), C: ee(c, f)}

    def t_of(xs, ls, cs):
        return xs * 4 + ls * 2 + cs

    def ys_dev(d, e):
        return {YH: yy(d), YL: ee(yl, e)}

    peers = [{Z: zz(d)} for d in zs]
    peers += [ys_dev(d, e) for d, e in ys] + [ts_dev(*v) for v in ts if v != (0, 1, 0)]
    barrier = pltpu.get_barrier_semaphore()
    for p in peers:
        pl.semaphore_signal(barrier, inc=1, device_id=p, device_id_type=MESH)

    loads = [
        (gout_h, gout), (tok_h, tok), (dw_h, w.at[0, z]), (gate_h, gu.at[0, k]),
        (up_h, gu.at[1, k]), (gw_h, w.at[1, z]), (uw_h, w.at[2, z]), (gain_h, gain),
    ]
    loads = [pltpu.make_async_copy(s, d, lsem.at[i]) for i, (s, d) in enumerate(loads)]
    for cp in loads:
        cp.start()

    loads[0].wait()
    for q in range(NY):
        for i in range(NZ):
            col = (i * NY + q) * 128
            st[0, q, :, i * 128:(i + 1) * 128] = gout[:, col:col + 128]
    a[0, k, x, yl, c] = st[0, k]
    loads[1].wait()
    tf = tok[...].astype(F32)
    inv = lax.rsqrt(jnp.mean(tf * tf, axis=1, keepdims=True) + 1e-05)
    irms[...] = jnp.broadcast_to(inv, (8, 128))
    for q in range(NY):
        for i in range(NZ):
            col = (i * NY + q) * 128
            st[1, q, :, i * 128:(i + 1) * 128] = (tf[:, col:col + 128] * inv).astype(BF)
    a[1, k, x, yl, c] = st[1, k]
    for cp in loads[2:]:
        cp.wait()
    pl.semaphore_wait(barrier, len(peers))

    def half(ref, h):
        return ref.at[pl.ds(224 * h, 224)]

    class Ring:
        def __init__(self, buf, at, me, n, left, right, sem, group):
            self.buf, self.at, self.me, self.n, self.sem, self.group = buf, at, me, n, sem, group
            self.devs = (right, left)

        def put(self, slot, way, step, h):
            p = half(self.buf.at[slot], h)
            send(p, p, self.devs[way], self.sem.at[way, step, h], self.group)

        def first(self):
            for i in range(2):
                for way in range(2):
                    self.put(self.me, way, 0, i ^ way)

        def got(self, s, way, h):
            slot = self.at(-s if way == 0 else s)
            arrived(half(self.buf.at[slot], h), self.sem.at[way, s - 1, h])
            return slot

        def nxt(self, s, parts=(0, 1)):
            for i in parts:
                for way in range(2):
                    slot = self.got(s, way, i ^ way)
                    if s + 1 < self.n // 2 or i == 0:
                        self.put(slot, way, s, i ^ way)

        def last(self):
            for way in range(2):
                self.got(self.n // 2, way, way)

    zl, zr, kl, kr = {Z: zz(-1)}, {Z: zz(1)}, {YH: yy(-1)}, {YH: yy(1)}
    dwr, gwr, uwr = [Ring(w.at[i], zz, z, NZ, zl, zr, wsem.at[i], "w%d" % i) for i in range(3)]
    gater, upr = [Ring(gu.at[i], yy, k, NY, kl, kr, gsem.at[i], "gu") for i in range(2)]
    gar = Ring(ga, yy, k, NY, kl, kr, gasem, "ga")
    core = {C: 1 - c}

    def s1_send(i):
        for d, e in ys:
            send(st.at[i, yy(d)], a.at[i, k, x, yl, c], ys_dev(d, e), s1sem.at[i], "s1")

    def s1_wait(i):
        arrived(units(7), s1sem.at[i])

    def unit(i, xs, cs):
        return a.at[i, :, xs, :, cs]

    def x_send(i):
        for d in (2, 1, 3):
            send(unit(i, x, c), unit(i, x, c), {X: xx(d)}, xsem.at[i, d], "x%d" % i)
        send(unit(i, x, c), unit(i, x, c), core, csem.at[i], "x%d" % i)

    def x_wait(i):
        for d in (1, 3, 2):
            u = unit(i, xx(-d), c)
            arrived(u, xsem.at[i, d])
            send(u, u, core, csem.at[i], "x%d" % i)

    def core_wait(i):
        arrived(units(32), csem.at[i])

    dwr.first()
    s1_send(0)
    s1_send(1)
    gater.first()
    upr.first()
    dwr.nxt(1)
    s1_wait(0)
    x_send(0)
    dwr.nxt(2)
    s1_wait(1)
    x_send(1)
    dwr.nxt(3)
    gwr.first()
    uwr.first()
    x_wait(0)
    dwr.last()
    core_wait(0)

    down = jnp.concatenate([w[0, i] for i in range(NZ)], axis=1)

    def partial(d, e):
        rows = [a.at[0, yy(v)].reshape(128, 1024)[...] for v in (d, e)]
        both = dot(down, jnp.concatenate(rows, axis=0), 1, 1)
        return both[:, :128], both[:, 128:]

    def own_half(n, dev, h):
        rows = slice(224 * h, 224 * h + 224)
        sa[2 * n, rows] = part[n, rows].astype(BF)
        send(half(sa.at[2 * n], h), half(ra.at[n], h), dev, rasem.at[n], "ga")

    far, part[0] = partial(2, 1)
    sa[1] = far.astype(BF)
    send(half(sa.at[1], 0), rb.at[0], kr, rbsem.at[0], "ga")
    send(half(sa.at[1], 1), rb.at[1], kl, rbsem.at[1], "ga")
    own_half(0, kr, 1)
    part[1], part[2] = partial(3, 0)
    own_half(1, kl, 0)

    gwr.nxt(1)
    uwr.nxt(1)
    x_wait(1)

    for n, (dev, h) in enumerate(((kr, 0), (kl, 1))):
        rows = slice(224 * h, 224 * h + 224)
        arrived(rb.at[n], rbsem.at[n])
        sa[2 * n, rows] = (part[n, rows] + rb[n].astype(F32)).astype(BF)
        send(half(sa.at[2 * n], h), half(ra.at[n], h), dev, rasem.at[n], "ga")
    gater.nxt(1)
    gwr.nxt(2)
    upr.nxt(1)
    core_wait(1)
    uwr.nxt(2)
    gwr.nxt(3)
    uwr.nxt(3)
    for n in range(2):
        arrived(ra.at[n], rasem.at[n])
    ga[k] = (part[2] + ra[0].astype(F32) + ra[1].astype(F32)).astype(BF)
    gar.first()

    gater.last()
    upr.last()
    for j in range(NY):
        gv = gu[0, j].astype(F32)
        uv = gu[1, j].astype(F32)
        sg = jax.nn.sigmoid(gv)
        sv = gv * sg
        fac[0, j] = uv * sg * (1.0 + gv * (1.0 - sg))
        fac[1, j] = sv
        act[j] = (sv * uv).astype(BF)

    acts = jnp.concatenate([act[j] for j in range(NY)], axis=1)
    rows_all = a.at[0].reshape(512, 1024)
    for i in range(NZ // 2):
        pair = dot(acts, rows_all[:, i * 256:(i + 1) * 256], 1, 0)
        ds_[2 * i] = pair[:, :128].astype(BF)
        ds_[2 * i + 1] = pair[:, 128:].astype(BF)

    def down_put(way, slot, step, h):
        send(
            half(ds_.at[slot], h), half(rd.at[way, step], h), (zr, zl)[way],
            rdsem.at[way, step, h], "down",
        )

    def down_add(way, slot, step, h):
        arrived(half(rd.at[way, step], h), rdsem.at[way, step, h])
        rows = slice(224 * h, 224 * h + 224)
        ds_[slot, rows] = (
            ds_[slot, rows].astype(F32) + rd[way, step, rows].astype(F32)
        ).astype(BF)

    def down_next(s):
        for i in range(2 if s > 1 else 1):
            for way in range(2):
                slot = zz(4 - s if way == 0 else s - 4)
                down_add(way, slot, s - 1, i ^ way)
                down_put(way, slot, s, i ^ way)

    for way in range(2):
        down_put(way, zz(4), 0, way)
    for way in range(2):
        down_put(way, zz(3 if way == 0 else -3), 1, 1 - way)

    gwr.last()
    uwr.last()

    def norm_part(d):
        j = yy(-d)
        gj = ga[j].astype(F32)
        both = jnp.concatenate([(gj * fac[0, j]).astype(BF), (gj * fac[1, j]).astype(BF)], axis=0)
        for i in range(NZ // 2):
            cols = jnp.concatenate(
                [
                    jnp.concatenate([w[1, 2 * i], w[2, 2 * i]], axis=0),
                    jnp.concatenate([w[1, 2 * i + 1], w[2, 2 * i + 1]], axis=0),
                ],
                axis=1,
            )
            block = dot(both, cols, 0, 0)
            lanes = slice(i * 256, (i + 1) * 256)
            for q in range(16):
                pn[d, q // 4, (q // 2) % 2, q % 2, :, lanes] = block[q * 8:(q + 1) * 8].astype(BF)
        send(pn.at[d, :, :, 1 - c], rc.at[d], core, rcsem.at[d], "norm")

    def norm_core(d):
        arrived(rc.at[d], rcsem.at[d])
        for i in range(NX):
            for j in range(2):
                sx[d, i, j] = (pn[d, i, j, c].astype(F32) + rc[d, i, j].astype(F32)).astype(BF)
        for e in (2, 1, 3):
            send(sx.at[d, xx(e)], rx.at[d, e], {X: xx(e)}, rxsem.at[d], "norm")

    def norm_x(d):
        arrived(units(6), rxsem.at[d])
        for f in (1, 0):
            v = ee(yl, f)
            rows = sx[d, x, v].astype(F32)
            for e in range(1, NX):
                rows = rows + rx[d, e, v].astype(F32)
            if d or f:
                fs[d, f] = rows.astype(BF)
                send(fs.at[d, f], fn.at[k, yl], ys_dev(-d, f), fnsem.at[0], "norm")
            else:
                fn[k, yl] = rows.astype(BF)

    def gain_part(d):
        add = gacc[...]
        for q in range(16):
            at = (q // 4, (q // 2) % 2, q % 2)
            add = add + pn[(d,) + at].astype(F32) * a[(1, yy(-d)) + at].astype(F32)
        gacc[...] = add

    gacc[...] = jnp.zeros((8, 1024), F32)
    norm_part(0)
    gar.nxt(1, (0,))
    norm_core(0)
    gar.nxt(1, (1,))
    norm_part(1)
    norm_part(3)
    down_next(1)
    norm_core(1)
    norm_core(3)
    for d in (0, 1, 3):
        gain_part(d)
    gar.last()
    norm_part(2)

    gain_part(2)
    mine = t_of(x, yl, c)
    for i in range(NZ):
        g1[mine, i:i + 1, :] = jnp.sum(gacc[:, i * 128:(i + 1) * 128], axis=0, keepdims=True)
    for d, e, f in ts:
        send(g1.at[mine], g1.at[mine], ts_dev(d, e, f), g1sem.at[0], "g1")

    norm_core(2)
    down_next(2)
    for d in (0, 1, 3):
        norm_x(d)
    arrived(g1.at[pl.ds(0, 15)], g1sem.at[0])
    g3[z] = jnp.sum(g1[...], axis=0)
    for d in zs:
        send(g3.at[z], g3.at[z], {Z: zz(d)}, g3sem.at[0], "g3")
    norm_x(2)
    down_next(3)

    arrived(g3.at[pl.ds(0, 7)], g3sem.at[0])
    g4[k] = jnp.sum(g3[...], axis=0)
    for d in (2, 1, 3):
        send(g4.at[k], g4.at[k], {YH: yy(d)}, g4sem.at[0], "g3")

    for h in range(2):
        for way in range(2):
            down_add(way, z, 3, h)
    outs = [pltpu.make_async_copy(ds_.at[z], dgrad, lsem.at[0])]
    outs[0].start()

    arrived(units(7), fnsem.at[0])
    for q in range(NY):
        gn[q] = fn[q, 0].astype(F32) + fn[q, 1].astype(F32)
    inv = irms[...]
    inner = jnp.zeros((8, 128), F32)
    for i in range(NZ):
        for q in range(NY):
            b = i * NY + q
            normed = tok[:, b * 128:(b + 1) * 128].astype(F32) * inv
            inner = inner + gn[q, :, i * 128:(i + 1) * 128] * gain[b:b + 1, :] * normed
    inner = jnp.sum(inner, axis=1, keepdims=True) * (1.0 / 4096)
    for i in range(NZ):
        for q in range(NY):
            b = i * NY + q
            cols = slice(b * 128, (b + 1) * 128)
            normed = tok[:, cols].astype(F32) * inv
            scaled = gn[q, :, i * 128:(i + 1) * 128] * gain[b:b + 1, :]
            tok[:, cols] = (
                gout[:, cols].astype(F32) + inv * (scaled - normed * inner)
            ).astype(BF)

    outs.append(pltpu.make_async_copy(tok, igrad, lsem.at[1]))
    outs[1].start()
    arrived(g4.at[pl.ds(0, 3)], g4sem.at[0])
    for i in range(NZ):
        for q in range(NY):
            b = i * NY + q
            gain[b:b + 1, :] = g4[q, i:i + 1, :]
    outs.append(pltpu.make_async_copy(gain, ggrad, lsem.at[2]))
    outs[2].start()
    sent = {
        "w0": w.at[0, pl.ds(0, 7)], "w1": w.at[0, pl.ds(0, 7)], "w2": w.at[0, pl.ds(0, 7)],
        "gu": w.at[0, pl.ds(0, 6)], "ga": w.at[0, pl.ds(0, 6)], "down": w.at[0, pl.ds(0, 7)],
        "s1": units(14), "x0": units(56), "x1": units(56), "norm": units(63),
        "g1": g1.at[pl.ds(0, 15)], "g3": g1.at[pl.ds(0, 10)],
    }
    for i, group in enumerate(sends):
        arrived(sent[group], ssem.at[i])
    for cp in outs:
        cp.wait()


def per_device(
    tokens_in, grad_out, gate_pre, up_pre, gate_weight, up_weight, down_weight, norm_gain
):
    vm = pltpu.VMEM
    dma = pltpu.SemaphoreType.DMA
    scratch = [
        vm((8, 4096), BF),
        vm((8, 4096), BF),
        vm((32, 128), F32),
        vm((3, NZ, 448, 128), BF),
        vm((2, NY, 448, 128), BF),
        vm((2, NY, NX, 2, 2, 8, 1024), BF),
        vm((2, NY, 8, 1024), BF),
        vm((2, NY, 448, 128), F32),
        vm((NY, 448, 128), BF),
        vm((3, 448, 128), BF),
        vm((2, 448, 128), BF),
        vm((2, 224, 128), BF),
        vm((3, 448, 128), F32),
        vm((NY, 448, 128), BF),
        vm((NY, NX, 2, 2, 8, 1024), BF),
        vm((NY, NX, 2, 8, 1024), BF),
        vm((NY, NX, 2, 8, 1024), BF),
        vm((NY, NX, 2, 8, 1024), BF),
        vm((NY, 2, 8, 1024), BF),
        vm((NY, 2, 8, 1024), BF),
        vm((NY, 8, 1024), F32),
        vm((NZ, 448, 128), BF),
        vm((2, 4, 448, 128), BF),
        vm((8, 1024), F32),
        vm((16, 8, 128), F32),
        vm((NZ, 8, 128), F32),
        vm((NY, 8, 128), F32),
        vm((8, 128), F32),
        dma((8,)),
        dma((12,)),
        dma((3, 2, 4, 2)),
        dma((2, 2, 2, 2)),
        dma((2,)),
        dma((2, 4)),
        dma((2,)),
        dma((2,)),
        dma((2,)),
        dma((2, 2, 2)),
        dma((4,)),
        dma((4,)),
        dma((1,)),
        dma((2, 4, 2)),
        dma((1,)),
        dma((1,)),
        dma((1,)),
    ]
    hbm = pl.BlockSpec(memory_space=pl.ANY)
    igrad, ggrad, dgrad = pl.pallas_call(
        kernel,
        out_shape=(
            jax.ShapeDtypeStruct((8, 4096), BF),
            jax.ShapeDtypeStruct((32, 128), F32),
            jax.ShapeDtypeStruct((448, 128), BF),
        ),
        in_specs=[hbm] * 8,
        out_specs=(hbm,) * 3,
        scratch_shapes=scratch,
        compiler_params=pltpu.CompilerParams(
            collective_id=0, has_side_effects=True, vmem_limit_bytes=60 * 1024 * 1024
        ),
    )(
        tokens_in, grad_out, gate_pre.T, up_pre.T, gate_weight.T, up_weight.T, down_weight,
        norm_gain.reshape(32, 128),
    )
    return igrad, ggrad.reshape(4096), dgrad


def solution(mesh):
    finer = Mesh(mesh.devices.reshape(NZ, NY, NX, 2, 2), AXES)
    return jax.shard_map(
        per_device,
        mesh=finer,
        in_specs=(
            P(AXES, None),
            P(AXES, None),
            P(DP, TENSOR),
            P(DP, TENSOR),
            P(DP, TENSOR),
            P(DP, TENSOR),
            P(TENSOR, DP),
            P(),
        ),
        out_specs=(P(AXES, None), P(), P(TENSOR, DP)),
        check_vma=False,
    )
```

```python
import jax
import jax.numpy as jnp
from jax import lax
from jax.experimental import pallas as pl
from jax.experimental.pallas import tpu as pltpu
from jax.sharding import Mesh
from jax.sharding import PartitionSpec as P

AXES = ("dp_0", "dp_1", "tensor_0", "tensor_1", "tensor_2")
Z, YH, X, YL, C = AXES
TENSOR = AXES[2:]
DP = AXES[:2]
BF = jnp.bfloat16
F32 = jnp.float32
MESH = pl.DeviceIdType.MESH
NZ, NY, NX = 8, 4, 4


def dot(a, b, ca, cb):
    return lax.dot_general(a, b, (((ca,), (cb,)), ((), ())), preferred_element_type=F32)


def kernel(
    tok_h, gout_h, gate_h, up_h, gw_h, uw_h, dw_h, gain_h,
    igrad, ggrad, dgrad,
    tok, gout, gain,
    w, gu, a, st, fac, act, sa, ra, rb, part, ga, pn, rc, sx, rx, fs, fn, gn, ds_, rd, gacc,
    g1, g3, g4, irms,
    lsem, ssem, wsem, gsem, s1sem, xsem, csem, rasem, rbsem, gasem, rcsem, rxsem, fnsem, rdsem,
    g1sem, g3sem, g4sem,
):
    z, k, x = lax.axis_index(Z), lax.axis_index(YH), lax.axis_index(X)
    yl, c = lax.axis_index(YL), lax.axis_index(C)
    sends = []

    def send(src, dst, dev, rsem, group):
        if group not in sends:
            sends.append(group)
        pltpu.make_async_remote_copy(
            src_ref=src, dst_ref=dst, send_sem=ssem.at[sends.index(group)], recv_sem=rsem,
            device_id=dev, device_id_type=MESH,
        ).start()

    def arrived(ref, rsem):
        pltpu.make_async_copy(ref, ref, rsem).wait()

    def units(n):
        return a.at[0].reshape(512, 1024).at[pl.ds(0, 8 * n)]

    def zz(d):
        return lax.rem(z + d + NZ, NZ)

    def yy(d):
        return lax.rem(k + d + NY, NY)

    def xx(d):
        return lax.rem(x + d + NX, NX)

    def ee(v, e):
        return lax.rem(v + e, 2)

    ys = [(d, e) for d in (2, 1, 3, 0) for e in (1, 0) if d or e]
    zs = (4, 3, 5, 2, 6, 1, 7)
    ts = [(d, e, f) for d in (2, 1, 3, 0) for e in (1, 0) for f in (1, 0) if d or e or f]

    def ts_dev(d, e, f):
        return {X: xx(d), YL: ee(yl, e), C: ee(c, f)}

    def t_of(xs, ls, cs):
        return xs * 4 + ls * 2 + cs

    def ys_dev(d, e):
        return {YH: yy(d), YL: ee(yl, e)}

    peers = [{Z: zz(d)} for d in zs]
    peers += [ys_dev(d, e) for d, e in ys] + [ts_dev(*v) for v in ts if v != (0, 1, 0)]
    loads = [
        (gout_h, gout), (tok_h, tok), (dw_h, w.at[0, z]), (gate_h, gu.at[0, k]),
        (up_h, gu.at[1, k]), (gw_h, w.at[1, z]), (uw_h, w.at[2, z]), (gain_h, gain),
    ]
    loads = [pltpu.make_async_copy(s, d, lsem.at[i]) for i, (s, d) in enumerate(loads)]
    for i in (0, 2, 3, 4, 1, 5, 6, 7):
        loads[i].start()
    barrier = pltpu.get_barrier_semaphore()
    for p in peers:
        pl.semaphore_signal(barrier, inc=1, device_id=p, device_id_type=MESH)

    loads[0].wait()
    for q in range(NY):
        for i in range(NZ):
            col = (i * NY + q) * 128
            st[0, q, :, i * 128:(i + 1) * 128] = gout[:, col:col + 128]
    loads[2].wait()
    pl.semaphore_wait(barrier, len(peers))

    def half(ref, h):
        return ref.at[pl.ds(224 * h, 224)]

    class Ring:
        def __init__(self, buf, at, me, n, left, right, sem, group):
            self.buf, self.at, self.me, self.n, self.sem, self.group = buf, at, me, n, sem, group
            self.devs = (right, left)

        def put(self, slot, way, step, h):
            p = half(self.buf.at[slot], h)
            send(p, p, self.devs[way], self.sem.at[way, step, h], self.group)

        def first(self):
            for i in range(2):
                for way in range(2):
                    self.put(self.me, way, 0, i ^ way)

        def got(self, s, way, h):
            slot = self.at(-s if way == 0 else s)
            arrived(half(self.buf.at[slot], h), self.sem.at[way, s - 1, h])
            return slot

        def nxt(self, s, parts=(0, 1)):
            for i in parts:
                for way in range(2):
                    slot = self.got(s, way, i ^ way)
                    if s + 1 < self.n // 2 or i == 0:
                        self.put(slot, way, s, i ^ way)

        def last(self):
            for way in range(2):
                self.got(self.n // 2, way, way)

    zl, zr, kl, kr = {Z: zz(-1)}, {Z: zz(1)}, {YH: yy(-1)}, {YH: yy(1)}
    dwr, gwr, uwr = [Ring(w.at[i], zz, z, NZ, zl, zr, wsem.at[i], "w%d" % i) for i in range(3)]
    gater, upr = [Ring(gu.at[i], yy, k, NY, kl, kr, gsem.at[i], "gu") for i in range(2)]
    gar = Ring(ga, yy, k, NY, kl, kr, gasem, "ga")
    core = {C: 1 - c}

    def s1_send(i):
        for d, e in ys:
            send(st.at[i, yy(d)], a.at[i, k, x, yl, c], ys_dev(d, e), s1sem.at[i], "s1")

    def s1_wait(i):
        arrived(units(7), s1sem.at[i])

    def unit(i, xs, cs):
        return a.at[i, :, xs, :, cs]

    def x_send(i):
        for d in (2, 1, 3):
            send(unit(i, x, c), unit(i, x, c), {X: xx(d)}, xsem.at[i, d], "x%d" % i)
        send(unit(i, x, c), unit(i, x, c), core, csem.at[i], "x%d" % i)

    def x_wait(i):
        for d in (1, 3, 2):
            u = unit(i, xx(-d), c)
            arrived(u, xsem.at[i, d])
            send(u, u, core, csem.at[i], "x%d" % i)

    def core_wait(i):
        arrived(units(32), csem.at[i])

    dwr.first()
    s1_send(0)
    for cp in loads[3:5]:
        cp.wait()
    gater.first()
    upr.first()
    a[0, k, x, yl, c] = st[0, k]

    loads[1].wait()
    tf = tok[...].astype(F32)
    inv = lax.rsqrt(jnp.mean(tf * tf, axis=1, keepdims=True) + 1e-05)
    irms[...] = jnp.broadcast_to(inv, (8, 128))
    for q in range(NY):
        for i in range(NZ):
            col = (i * NY + q) * 128
            st[1, q, :, i * 128:(i + 1) * 128] = (tf[:, col:col + 128] * inv).astype(BF)
    a[1, k, x, yl, c] = st[1, k]
    s1_send(1)
    for cp in loads[5:]:
        cp.wait()

    dwr.nxt(1)
    s1_wait(0)
    x_send(0)
    dwr.nxt(2)
    dwr.nxt(3)
    gwr.first()
    uwr.first()
    x_wait(0)
    dwr.last()
    gater.nxt(1)
    core_wait(0)

    down = jnp.concatenate([w[0, i] for i in range(NZ)], axis=1)

    def partial(d, e):
        rows = [a.at[0, yy(v)].reshape(128, 1024)[...] for v in (d, e)]
        both = dot(down, jnp.concatenate(rows, axis=0), 1, 1)
        return both[:, :128], both[:, 128:]

    def own_half(n, dev, h):
        rows = slice(224 * h, 224 * h + 224)
        sa[2 * n, rows] = part[n, rows].astype(BF)
        send(half(sa.at[2 * n], h), half(ra.at[n], h), dev, rasem.at[n], "ga")

    far, part[0] = partial(2, 1)
    sa[1] = far.astype(BF)
    send(half(sa.at[1], 0), rb.at[0], kr, rbsem.at[0], "ga")
    send(half(sa.at[1], 1), rb.at[1], kl, rbsem.at[1], "ga")
    own_half(0, kr, 1)
    part[1], part[2] = partial(3, 0)
    own_half(1, kl, 0)

    gwr.nxt(1)
    uwr.nxt(1)
    s1_wait(1)
    x_send(1)

    for n, (dev, h) in enumerate(((kr, 0), (kl, 1))):
        rows = slice(224 * h, 224 * h + 224)
        arrived(rb.at[n], rbsem.at[n])
        sa[2 * n, rows] = (part[n, rows] + rb[n].astype(F32)).astype(BF)
        send(half(sa.at[2 * n], h), half(ra.at[n], h), dev, rasem.at[n], "ga")
    upr.nxt(1)
    gwr.nxt(2)
    uwr.nxt(2)
    x_wait(1)
    gwr.nxt(3)
    for n in range(2):
        arrived(ra.at[n], rasem.at[n])
    ga[k] = (part[2] + ra[0].astype(F32) + ra[1].astype(F32)).astype(BF)
    gar.first()

    gater.last()
    upr.last()
    for j in range(NY):
        gv = gu[0, j].astype(F32)
        uv = gu[1, j].astype(F32)
        sg = jax.nn.sigmoid(gv)
        sv = gv * sg
        fac[0, j] = uv * sg * (1.0 + gv * (1.0 - sg))
        fac[1, j] = sv
        act[j] = (sv * uv).astype(BF)
    uwr.nxt(3)

    acts = jnp.concatenate([act[j] for j in range(NY)], axis=1)
    rows_all = a.at[0].reshape(512, 1024)
    for i in range(NZ // 2):
        pair = dot(acts, rows_all[:, i * 256:(i + 1) * 256], 1, 0)
        ds_[2 * i] = pair[:, :128].astype(BF)
        ds_[2 * i + 1] = pair[:, 128:].astype(BF)

    def down_put(way, slot, step, h):
        send(
            half(ds_.at[slot], h), half(rd.at[way, step], h), (zr, zl)[way],
            rdsem.at[way, step, h], "down",
        )

    def down_add(way, slot, step, h):
        arrived(half(rd.at[way, step], h), rdsem.at[way, step, h])
        rows = slice(224 * h, 224 * h + 224)
        ds_[slot, rows] = (
            ds_[slot, rows].astype(F32) + rd[way, step, rows].astype(F32)
        ).astype(BF)

    def down_next(s):
        for i in range(2 if s > 1 else 1):
            for way in range(2):
                slot = zz(4 - s if way == 0 else s - 4)
                down_add(way, slot, s - 1, i ^ way)
                down_put(way, slot, s, i ^ way)

    for way in range(2):
        down_put(way, zz(4), 0, way)
    for way in range(2):
        down_put(way, zz(3 if way == 0 else -3), 1, 1 - way)

    def norm_part(d):
        j = yy(-d)
        gj = ga[j].astype(F32)
        both = jnp.concatenate([(gj * fac[0, j]).astype(BF), (gj * fac[1, j]).astype(BF)], axis=0)
        for i in range(NZ // 2):
            cols = jnp.concatenate(
                [
                    jnp.concatenate([w[1, 2 * i], w[2, 2 * i]], axis=0),
                    jnp.concatenate([w[1, 2 * i + 1], w[2, 2 * i + 1]], axis=0),
                ],
                axis=1,
            )
            block = dot(both, cols, 0, 0)
            lanes = slice(i * 256, (i + 1) * 256)
            for q in range(16):
                pn[d, q // 4, (q // 2) % 2, q % 2, :, lanes] = block[q * 8:(q + 1) * 8].astype(BF)
        send(pn.at[d, :, :, 1 - c], rc.at[d], core, rcsem.at[d], "norm")

    def norm_core(d):
        arrived(rc.at[d], rcsem.at[d])
        for i in range(NX):
            for j in range(2):
                sx[d, i, j] = (pn[d, i, j, c].astype(F32) + rc[d, i, j].astype(F32)).astype(BF)
        for e in (2, 1, 3):
            send(sx.at[d, xx(e)], rx.at[d, e], {X: xx(e)}, rxsem.at[d], "norm")

    def norm_x(d):
        arrived(units(6), rxsem.at[d])
        for f in (1, 0):
            v = ee(yl, f)
            rows = sx[d, x, v].astype(F32)
            for e in range(1, NX):
                rows = rows + rx[d, e, v].astype(F32)
            if d or f:
                fs[d, f] = rows.astype(BF)
                send(fs.at[d, f], fn.at[k, yl], ys_dev(-d, f), fnsem.at[0], "norm")
            else:
                fn[k, yl] = rows.astype(BF)

    def gain_part(d):
        add = gacc[...]
        for q in range(16):
            at = (q // 4, (q // 2) % 2, q % 2)
            add = add + pn[(d,) + at].astype(F32) * a[(1, yy(-d)) + at].astype(F32)
        gacc[...] = add

    gacc[...] = jnp.zeros((8, 1024), F32)
    gar.nxt(1, (0,))
    gwr.last()
    uwr.last()
    norm_part(0)
    gar.nxt(1, (1,))
    norm_part(1)
    norm_part(3)
    norm_core(0)
    down_next(1)
    core_wait(1)
    for d in (0, 1, 3):
        gain_part(d)
    gar.last()
    norm_part(2)

    gain_part(2)
    mine = t_of(x, yl, c)
    for i in range(NZ):
        g1[mine, i:i + 1, :] = jnp.sum(gacc[:, i * 128:(i + 1) * 128], axis=0, keepdims=True)
    for d, e, f in ts:
        send(g1.at[mine], g1.at[mine], ts_dev(d, e, f), g1sem.at[0], "g1")

    for d in (1, 3, 2):
        norm_core(d)
    norm_x(0)
    down_next(2)
    arrived(g1.at[pl.ds(0, 15)], g1sem.at[0])

    @pl.when(c == 1)
    def _():
        g3[z] = jnp.sum(g1[...], axis=0)
        for d in zs:
            send(g3.at[z], g3.at[z], {Z: zz(d)}, g3sem.at[0], "g3")

    for d in (1, 3, 2):
        norm_x(d)
    down_next(3)

    @pl.when(c == 1)
    def _():
        arrived(g3.at[pl.ds(0, 7)], g3sem.at[0])
        g4[k] = jnp.sum(g3[...], axis=0)
        for d in (2, 1, 3):
            send(g4.at[k], g4.at[k], {YH: yy(d)}, g4sem.at[0], "g3")

    for h in range(2):
        for way in range(2):
            down_add(way, z, 3, h)
    outs = [pltpu.make_async_copy(ds_.at[z], dgrad, lsem.at[0])]
    outs[0].start()

    arrived(units(7), fnsem.at[0])
    for q in range(NY):
        gn[q] = fn[q, 0].astype(F32) + fn[q, 1].astype(F32)
    inv = irms[...]
    inner = jnp.zeros((8, 128), F32)
    for i in range(NZ):
        for q in range(NY):
            b = i * NY + q
            normed = tok[:, b * 128:(b + 1) * 128].astype(F32) * inv
            inner = inner + gn[q, :, i * 128:(i + 1) * 128] * gain[b:b + 1, :] * normed
    inner = jnp.sum(inner, axis=1, keepdims=True) * (1.0 / 4096)
    for i in range(NZ):
        for q in range(NY):
            b = i * NY + q
            cols = slice(b * 128, (b + 1) * 128)
            normed = tok[:, cols].astype(F32) * inv
            scaled = gn[q, :, i * 128:(i + 1) * 128] * gain[b:b + 1, :]
            tok[:, cols] = (
                gout[:, cols].astype(F32) + inv * (scaled - normed * inner)
            ).astype(BF)

    outs.append(pltpu.make_async_copy(tok, igrad, lsem.at[1]))
    outs[1].start()

    @pl.when(c == 1)
    def _():
        arrived(g4.at[pl.ds(0, 3)], g4sem.at[0])
        send(g4, g4, core, g4sem.at[1], "g4")

    @pl.when(c == 0)
    def _():
        arrived(g4, g4sem.at[1])

    for i in range(NZ):
        for q in range(NY):
            b = i * NY + q
            gain[b:b + 1, :] = g4[q, i:i + 1, :]
    outs.append(pltpu.make_async_copy(gain, ggrad, lsem.at[2]))
    outs[2].start()
    sent = {
        "w0": w.at[0, pl.ds(0, 7)], "w1": w.at[0, pl.ds(0, 7)], "w2": w.at[0, pl.ds(0, 7)],
        "gu": w.at[0, pl.ds(0, 6)], "ga": w.at[0, pl.ds(0, 6)], "down": w.at[0, pl.ds(0, 7)],
        "s1": units(14), "x0": units(56), "x1": units(56), "norm": units(63),
        "g1": g1.at[pl.ds(0, 15)], "g3": g1.at[pl.ds(0, 10)], "g4": g4,
    }

    def all_sent(late):
        for i, group in enumerate(sends):
            if (group in ("g3", "g4")) == late:
                arrived(sent[group], ssem.at[i])

    all_sent(False)

    @pl.when(c == 1)
    def _():
        all_sent(True)

    for cp in outs:
        cp.wait()


def hand_on(i0, i1, i2, o0, o1, o2, b0, b1, b2, sem):
    ins = [pltpu.make_async_copy(s, d, sem.at[0, n]) for n, (s, d) in enumerate(((i0, b0), (i1, b1), (i2, b2)))]
    outs = [pltpu.make_async_copy(s, d, sem.at[1, n]) for n, (s, d) in enumerate(((b0, o0), (b1, o1), (b2, o2)))]
    for cp in ins:
        cp.start()
    for i, o in zip(ins, outs):
        i.wait()
        o.start()
    for cp in outs:
        cp.wait()


def per_device(
    tokens_in, grad_out, gate_pre, up_pre, gate_weight, up_weight, down_weight, norm_gain
):
    vm = pltpu.VMEM
    dma = pltpu.SemaphoreType.DMA
    scratch = [
        vm((8, 4096), BF),
        vm((8, 4096), BF),
        vm((32, 128), F32),
        vm((3, NZ, 448, 128), BF),
        vm((2, NY, 448, 128), BF),
        vm((2, NY, NX, 2, 2, 8, 1024), BF),
        vm((2, NY, 8, 1024), BF),
        vm((2, NY, 448, 128), F32),
        vm((NY, 448, 128), BF),
        vm((3, 448, 128), BF),
        vm((2, 448, 128), BF),
        vm((2, 224, 128), BF),
        vm((3, 448, 128), F32),
        vm((NY, 448, 128), BF),
        vm((NY, NX, 2, 2, 8, 1024), BF),
        vm((NY, NX, 2, 8, 1024), BF),
        vm((NY, NX, 2, 8, 1024), BF),
        vm((NY, NX, 2, 8, 1024), BF),
        vm((NY, 2, 8, 1024), BF),
        vm((NY, 2, 8, 1024), BF),
        vm((NY, 8, 1024), F32),
        vm((NZ, 448, 128), BF),
        vm((2, 4, 448, 128), BF),
        vm((8, 1024), F32),
        vm((16, 8, 128), F32),
        vm((NZ, 8, 128), F32),
        vm((NY, 8, 128), F32),
        vm((8, 128), F32),
        dma((8,)),
        dma((13,)),
        dma((3, 2, 4, 2)),
        dma((2, 2, 2, 2)),
        dma((2,)),
        dma((2, 4)),
        dma((2,)),
        dma((2,)),
        dma((2,)),
        dma((2, 2, 2)),
        dma((4,)),
        dma((4,)),
        dma((1,)),
        dma((2, 4, 2)),
        dma((1,)),
        dma((1,)),
        dma((2,)),
    ]
    hbm = pl.BlockSpec(memory_space=pl.ANY)
    shapes = (
        jax.ShapeDtypeStruct((8, 4096), BF),
        jax.ShapeDtypeStruct((32, 128), F32),
        jax.ShapeDtypeStruct((448, 128), BF),
    )
    results = pl.pallas_call(
        kernel,
        out_shape=shapes,
        in_specs=[hbm] * 8,
        out_specs=(hbm,) * 3,
        scratch_shapes=scratch,
        compiler_params=pltpu.CompilerParams(
            collective_id=0, has_side_effects=True, vmem_limit_bytes=60 * 1024 * 1024
        ),
    )(
        tokens_in, grad_out, gate_pre.T, up_pre.T, gate_weight.T, up_weight.T, down_weight,
        norm_gain.reshape(32, 128),
    )
    igrad, ggrad, dgrad = pl.pallas_call(
        hand_on,
        out_shape=shapes,
        in_specs=[hbm] * 3,
        out_specs=(hbm,) * 3,
        scratch_shapes=[vm(v.shape, v.dtype) for v in shapes] + [dma((2, 3))],
        compiler_params=pltpu.CompilerParams(vmem_limit_bytes=60 * 1024 * 1024),
    )(*results)
    return igrad, ggrad.reshape(4096), dgrad


def solution(mesh):
    finer = Mesh(mesh.devices.reshape(NZ, NY, NX, 2, 2), AXES)
    return jax.shard_map(
        per_device,
        mesh=finer,
        in_specs=(
            P(AXES, None),
            P(AXES, None),
            P(DP, TENSOR),
            P(DP, TENSOR),
            P(DP, TENSOR),
            P(DP, TENSOR),
            P(TENSOR, DP),
            P(),
        ),
        out_specs=(P(AXES, None), P(), P(TENSOR, DP)),
        check_vma=False,
    )
```

```python
import jax
import jax.numpy as jnp
from jax import lax
from jax.experimental import pallas as pl
from jax.experimental.pallas import tpu as pltpu
from jax.sharding import Mesh
from jax.sharding import PartitionSpec as P

AXES = ("dp_0", "dp_1", "tensor_0", "tensor_1", "tensor_2")
Z, YH, X, YL, C = AXES
TENSOR = AXES[2:]
DP = AXES[:2]
BF = jnp.bfloat16
F32 = jnp.float32
MESH = pl.DeviceIdType.MESH
NZ, NY, NX = 8, 4, 4


def dot(a, b, ca, cb):
    return lax.dot_general(a, b, (((ca,), (cb,)), ((), ())), preferred_element_type=F32)


def kernel(
    tok_h, gout_h, gate_h, up_h, gw_h, uw_h, dw_h, gain_h,
    igrad, ggrad, dgrad,
    tok, gout, gain,
    w, gu, a, st, fac, act, sa, ra, rb, part, ga, pn, rc, sx, rx, fs, fn, gn, ds_, rd, gacc,
    g1, g3, g4, irms,
    lsem, ssem, wsem, gsem, s1sem, xsem, csem, rasem, rbsem, gasem, rcsem, rxsem, fnsem, rdsem,
    g1sem, g3sem, g4sem,
):
    z, k, x = lax.axis_index(Z), lax.axis_index(YH), lax.axis_index(X)
    yl, c = lax.axis_index(YL), lax.axis_index(C)
    sends = []

    def send(src, dst, dev, rsem, group):
        if group not in sends:
            sends.append(group)
        pltpu.make_async_remote_copy(
            src_ref=src, dst_ref=dst, send_sem=ssem.at[sends.index(group)], recv_sem=rsem,
            device_id=dev, device_id_type=MESH,
        ).start()

    def arrived(ref, rsem):
        pltpu.make_async_copy(ref, ref, rsem).wait()

    def units(n):
        return a.at[0].reshape(512, 1024).at[pl.ds(0, 8 * n)]

    def zz(d):
        return lax.rem(z + d + NZ, NZ)

    def yy(d):
        return lax.rem(k + d + NY, NY)

    def xx(d):
        return lax.rem(x + d + NX, NX)

    def ee(v, e):
        return lax.rem(v + e, 2)

    ys = [(d, e) for d in (2, 1, 3, 0) for e in (1, 0) if d or e]
    zs = (4, 3, 5, 2, 6, 1, 7, 0)
    dps = [(d, e) for d in zs for e in (2, 1, 3, 0) if d or e]
    ts = [(d, e, f) for d in (2, 1, 3, 0) for e in (1, 0) for f in (1, 0) if d or e or f]

    def ts_dev(d, e, f):
        return {X: xx(d), YL: ee(yl, e), C: ee(c, f)}

    def t_of(xs, ls, cs):
        return xs * 4 + ls * 2 + cs

    def ys_dev(d, e):
        return {YH: yy(d), YL: ee(yl, e)}

    peers = [{Z: zz(1)}, {Z: zz(-1)}] + [ys_dev(d, e) for d, e in ys]
    peers += [{X: xx(d)} for d in (2, 1, 3)] + [{C: 1 - c}]
    loads = [
        (gout_h, gout), (tok_h, tok), (dw_h, w.at[0, z]), (gate_h, gu.at[0, k]),
        (up_h, gu.at[1, k]), (gw_h, w.at[1, z]), (uw_h, w.at[2, z]), (gain_h, gain),
    ]
    loads = [pltpu.make_async_copy(s, d, lsem.at[i]) for i, (s, d) in enumerate(loads)]
    for i in (0, 2, 3, 4, 1, 5, 6, 7):
        loads[i].start()
    barrier = pltpu.get_barrier_semaphore()
    for p in peers:
        pl.semaphore_signal(barrier, inc=1, device_id=p, device_id_type=MESH)

    loads[0].wait()
    for q in range(NY):
        for i in range(NZ):
            col = (i * NY + q) * 128
            st[0, q, :, i * 128:(i + 1) * 128] = gout[:, col:col + 128]
    loads[2].wait()
    pl.semaphore_wait(barrier, len(peers))

    def half(ref, h):
        return ref.at[pl.ds(224 * h, 224)]

    class Ring:
        def __init__(self, buf, at, me, n, left, right, sem, group):
            self.buf, self.at, self.me, self.n, self.sem, self.group = buf, at, me, n, sem, group
            self.devs = (right, left)

        def put(self, slot, way, step, h):
            p = half(self.buf.at[slot], h)
            send(p, p, self.devs[way], self.sem.at[way, step, h], self.group)

        def first(self):
            for i in range(2):
                for way in range(2):
                    self.put(self.me, way, 0, i ^ way)

        def got(self, s, way, h):
            slot = self.at(-s if way == 0 else s)
            arrived(half(self.buf.at[slot], h), self.sem.at[way, s - 1, h])
            return slot

        def nxt(self, s, parts=(0, 1)):
            for i in parts:
                for way in range(2):
                    slot = self.got(s, way, i ^ way)
                    if s + 1 < self.n // 2 or i == 0:
                        self.put(slot, way, s, i ^ way)

        def last(self):
            for way in range(2):
                self.got(self.n // 2, way, way)

    zl, zr, kl, kr = {Z: zz(-1)}, {Z: zz(1)}, {YH: yy(-1)}, {YH: yy(1)}
    dwr, gwr, uwr = [Ring(w.at[i], zz, z, NZ, zl, zr, wsem.at[i], "w%d" % i) for i in range(3)]
    gater, upr = [Ring(gu.at[i], yy, k, NY, kl, kr, gsem.at[i], "gu") for i in range(2)]
    gar = Ring(ga, yy, k, NY, kl, kr, gasem, "ga")
    core = {C: 1 - c}

    def s1_send(i):
        for d, e in ys:
            send(st.at[i, yy(d)], a.at[i, k, x, yl, c], ys_dev(d, e), s1sem.at[i], "s1")

    def s1_wait(i):
        arrived(units(7), s1sem.at[i])

    def unit(i, xs, cs):
        return a.at[i, :, xs, :, cs]

    def x_send(i):
        for d in (2, 1, 3):
            send(unit(i, x, c), unit(i, x, c), {X: xx(d)}, xsem.at[i, d], "x%d" % i)
        send(unit(i, x, c), unit(i, x, c), core, csem.at[i], "x%d" % i)

    def x_wait(i):
        for d in (1, 3, 2):
            u = unit(i, xx(-d), c)
            arrived(u, xsem.at[i, d])
            send(u, u, core, csem.at[i], "x%d" % i)

    def core_wait(i):
        arrived(units(32), csem.at[i])

    dwr.first()
    s1_send(0)
    for cp in loads[3:5]:
        cp.wait()
    gater.first()
    upr.first()
    a[0, k, x, yl, c] = st[0, k]

    loads[1].wait()
    tf = tok[...].astype(F32)
    inv = lax.rsqrt(jnp.mean(tf * tf, axis=1, keepdims=True) + 1e-05)
    irms[...] = jnp.broadcast_to(inv, (8, 128))
    for q in range(NY):
        for i in range(NZ):
            col = (i * NY + q) * 128
            st[1, q, :, i * 128:(i + 1) * 128] = (tf[:, col:col + 128] * inv).astype(BF)
    a[1, k, x, yl, c] = st[1, k]
    s1_send(1)
    for cp in loads[5:]:
        cp.wait()

    dwr.nxt(1)
    s1_wait(0)
    x_send(0)
    dwr.nxt(2)
    dwr.nxt(3)
    gwr.first()
    uwr.first()
    x_wait(0)
    dwr.last()
    gater.nxt(1)
    core_wait(0)

    down = jnp.concatenate([w[0, i] for i in range(NZ)], axis=1)

    def partial(d, e):
        rows = [a.at[0, yy(v)].reshape(128, 1024)[...] for v in (d, e)]
        both = dot(down, jnp.concatenate(rows, axis=0), 1, 1)
        return both[:, :128], both[:, 128:]

    def own_half(n, dev, h):
        rows = slice(224 * h, 224 * h + 224)
        sa[2 * n, rows] = part[n, rows].astype(BF)
        send(half(sa.at[2 * n], h), half(ra.at[n], h), dev, rasem.at[n], "ga")

    far, part[0] = partial(2, 1)
    sa[1] = far.astype(BF)
    send(half(sa.at[1], 0), rb.at[0], kr, rbsem.at[0], "ga")
    send(half(sa.at[1], 1), rb.at[1], kl, rbsem.at[1], "ga")
    own_half(0, kr, 1)
    part[1], part[2] = partial(3, 0)
    own_half(1, kl, 0)

    gwr.nxt(1)
    uwr.nxt(1)
    s1_wait(1)
    x_send(1)

    for n, (dev, h) in enumerate(((kr, 0), (kl, 1))):
        rows = slice(224 * h, 224 * h + 224)
        arrived(rb.at[n], rbsem.at[n])
        sa[2 * n, rows] = (part[n, rows] + rb[n].astype(F32)).astype(BF)
        send(half(sa.at[2 * n], h), half(ra.at[n], h), dev, rasem.at[n], "ga")
    upr.nxt(1)
    gwr.nxt(2)
    uwr.nxt(2)
    x_wait(1)
    gwr.nxt(3)
    for n in range(2):
        arrived(ra.at[n], rasem.at[n])
    ga[k] = (part[2] + ra[0].astype(F32) + ra[1].astype(F32)).astype(BF)
    gar.first()

    gater.last()
    upr.last()
    for j in range(NY):
        gv = gu[0, j].astype(F32)
        uv = gu[1, j].astype(F32)
        sg = jax.nn.sigmoid(gv)
        sv = gv * sg
        fac[0, j] = uv * sg * (1.0 + gv * (1.0 - sg))
        fac[1, j] = sv
        act[j] = (sv * uv).astype(BF)
    uwr.nxt(3)

    acts = jnp.concatenate([act[j] for j in range(NY)], axis=1)
    rows_all = a.at[0].reshape(512, 1024)
    for i in range(NZ // 2):
        pair = dot(acts, rows_all[:, i * 256:(i + 1) * 256], 1, 0)
        ds_[2 * i] = pair[:, :128].astype(BF)
        ds_[2 * i + 1] = pair[:, 128:].astype(BF)

    def down_put(way, slot, step, h):
        send(
            half(ds_.at[slot], h), half(rd.at[way, step], h), (zr, zl)[way],
            rdsem.at[way, step, h], "down",
        )

    def down_add(way, slot, step, h):
        arrived(half(rd.at[way, step], h), rdsem.at[way, step, h])
        rows = slice(224 * h, 224 * h + 224)
        ds_[slot, rows] = (
            ds_[slot, rows].astype(F32) + rd[way, step, rows].astype(F32)
        ).astype(BF)

    def down_next(s, i):
        for way in range(2):
            slot = zz(4 - s if way == 0 else s - 4)
            down_add(way, slot, s - 1, i ^ way)
            if s < 4:
                down_put(way, slot, s, i ^ way)

    for way in range(2):
        down_put(way, zz(4), 0, way)
    for way in range(2):
        down_put(way, zz(3 if way == 0 else -3), 1, 1 - way)

    def norm_part(d):
        j = yy(-d)
        gj = ga[j].astype(F32)
        both = jnp.concatenate([(gj * fac[0, j]).astype(BF), (gj * fac[1, j]).astype(BF)], axis=0)
        for i in range(NZ // 2):
            cols = jnp.concatenate(
                [
                    jnp.concatenate([w[1, 2 * i], w[2, 2 * i]], axis=0),
                    jnp.concatenate([w[1, 2 * i + 1], w[2, 2 * i + 1]], axis=0),
                ],
                axis=1,
            )
            block = dot(both, cols, 0, 0)
            lanes = slice(i * 256, (i + 1) * 256)
            for q in range(16):
                pn[d, q // 4, (q // 2) % 2, q % 2, :, lanes] = block[q * 8:(q + 1) * 8].astype(BF)
        send(pn.at[d, :, :, 1 - c], rc.at[d], core, rcsem.at[d], "norm")

    def norm_core(d):
        arrived(rc.at[d], rcsem.at[d])
        for i in range(NX):
            for j in range(2):
                sx[d, i, j] = (pn[d, i, j, c].astype(F32) + rc[d, i, j].astype(F32)).astype(BF)
        for e in (2, 1, 3):
            send(sx.at[d, xx(e)], rx.at[d, e], {X: xx(e)}, rxsem.at[d], "norm")

    def norm_x(d):
        arrived(units(6), rxsem.at[d])
        for f in (1, 0):
            v = ee(yl, f)
            rows = sx[d, x, v].astype(F32)
            for e in range(1, NX):
                rows = rows + rx[d, e, v].astype(F32)
            if d or f:
                fs[d, f] = rows.astype(BF)
                send(fs.at[d, f], fn.at[k, yl], ys_dev(-d, f), fnsem.at[0], "norm")
            else:
                fn[k, yl] = rows.astype(BF)

    def gain_part(d):
        add = gacc[...]
        for q in range(16):
            at = (q // 4, (q // 2) % 2, q % 2)
            add = add + pn[(d,) + at].astype(F32) * a[(1, yy(-d)) + at].astype(F32)
        gacc[...] = add

    gacc[...] = jnp.zeros((8, 1024), F32)
    gar.nxt(1, (0,))
    gwr.last()
    uwr.last()
    norm_part(0)
    gar.nxt(1, (1,))
    norm_part(1)
    norm_part(3)
    norm_core(0)
    norm_core(1)
    down_next(1, 0)
    down_next(2, 1)
    core_wait(1)
    for d in (0, 1, 3):
        gain_part(d)
    gar.last()
    norm_part(2)

    gain_part(2)
    mine = t_of(x, yl, c)
    for i in range(NZ):
        g1[mine, i:i + 1, :] = jnp.sum(gacc[:, i * 128:(i + 1) * 128], axis=0, keepdims=True)
    for d, e, f in ts:
        send(g1.at[mine], g1.at[mine], ts_dev(d, e, f), g1sem.at[0], "g1")

    norm_core(2)
    norm_core(3)
    down_next(2, 0)
    down_next(3, 1)
    norm_x(0)
    norm_x(1)
    arrived(g1.at[pl.ds(0, 15)], g1sem.at[0])

    @pl.when(c == 1)
    def _():
        g3[z * NY + k] = jnp.sum(g1[...], axis=0)
        for d, e in dps:
            send(
                g3.at[z * NY + k], g3.at[z * NY + k], {Z: zz(d), YH: yy(e)}, g3sem.at[0], "g3"
            )

    norm_x(2)
    norm_x(3)
    down_next(3, 0)
    down_next(4, 1)


    down_next(4, 0)
    outs = [pltpu.make_async_copy(ds_.at[z], dgrad, lsem.at[0])]
    outs[0].start()

    arrived(units(7), fnsem.at[0])
    for q in range(NY):
        gn[q] = fn[q, 0].astype(F32) + fn[q, 1].astype(F32)
    inv = irms[...]
    inner = jnp.zeros((8, 128), F32)
    for i in range(NZ):
        for q in range(NY):
            b = i * NY + q
            normed = tok[:, b * 128:(b + 1) * 128].astype(F32) * inv
            inner = inner + gn[q, :, i * 128:(i + 1) * 128] * gain[b:b + 1, :] * normed
    inner = jnp.sum(inner, axis=1, keepdims=True) * (1.0 / 4096)
    for i in range(NZ):
        for q in range(NY):
            b = i * NY + q
            cols = slice(b * 128, (b + 1) * 128)
            normed = tok[:, cols].astype(F32) * inv
            scaled = gn[q, :, i * 128:(i + 1) * 128] * gain[b:b + 1, :]
            tok[:, cols] = (
                gout[:, cols].astype(F32) + inv * (scaled - normed * inner)
            ).astype(BF)

    outs.append(pltpu.make_async_copy(tok, igrad, lsem.at[1]))
    outs[1].start()

    @pl.when(c == 1)
    def _():
        arrived(g3.at[pl.ds(0, 31)], g3sem.at[0])
        for q in range(NY):
            total = g3[q]
            for i in range(1, NZ):
                total = total + g3[i * NY + q]
            g4[q] = total
        send(g4, g4, core, g4sem.at[0], "g4")

    @pl.when(c == 0)
    def _():
        arrived(g4, g4sem.at[0])

    for i in range(NZ):
        for q in range(NY):
            b = i * NY + q
            gain[b:b + 1, :] = g4[q, i:i + 1, :]
    outs.append(pltpu.make_async_copy(gain, ggrad, lsem.at[2]))
    outs[2].start()
    sent = {
        "w0": w.at[0, pl.ds(0, 7)], "w1": w.at[0, pl.ds(0, 7)], "w2": w.at[0, pl.ds(0, 7)],
        "gu": w.at[0, pl.ds(0, 6)], "ga": w.at[0, pl.ds(0, 6)], "down": w.at[0, pl.ds(0, 7)],
        "s1": units(14), "x0": units(56), "x1": units(56), "norm": units(63),
        "g1": g1.at[pl.ds(0, 15)], "g3": g3.at[pl.ds(0, 31)], "g4": g4,
    }

    def all_sent(late):
        for i, group in enumerate(sends):
            if (group in ("g3", "g4")) == late:
                arrived(sent[group], ssem.at[i])

    all_sent(False)

    @pl.when(c == 1)
    def _():
        all_sent(True)

    for cp in outs:
        cp.wait()


def hand_on(i0, i1, i2, o0, o1, o2, b0, b1, b2, sem):
    ins = [pltpu.make_async_copy(s, d, sem.at[0, n]) for n, (s, d) in enumerate(((i0, b0), (i1, b1), (i2, b2)))]
    outs = [pltpu.make_async_copy(s, d, sem.at[1, n]) for n, (s, d) in enumerate(((b0, o0), (b1, o1), (b2, o2)))]
    for cp in ins:
        cp.start()
    for i, o in zip(ins, outs):
        i.wait()
        o.start()
    for cp in outs:
        cp.wait()


def per_device(
    tokens_in, grad_out, gate_pre, up_pre, gate_weight, up_weight, down_weight, norm_gain
):
    vm = pltpu.VMEM
    dma = pltpu.SemaphoreType.DMA
    scratch = [
        vm((8, 4096), BF),
        vm((8, 4096), BF),
        vm((32, 128), F32),
        vm((3, NZ, 448, 128), BF),
        vm((2, NY, 448, 128), BF),
        vm((2, NY, NX, 2, 2, 8, 1024), BF),
        vm((2, NY, 8, 1024), BF),
        vm((2, NY, 448, 128), F32),
        vm((NY, 448, 128), BF),
        vm((3, 448, 128), BF),
        vm((2, 448, 128), BF),
        vm((2, 224, 128), BF),
        vm((3, 448, 128), F32),
        vm((NY, 448, 128), BF),
        vm((NY, NX, 2, 2, 8, 1024), BF),
        vm((NY, NX, 2, 8, 1024), BF),
        vm((NY, NX, 2, 8, 1024), BF),
        vm((NY, NX, 2, 8, 1024), BF),
        vm((NY, 2, 8, 1024), BF),
        vm((NY, 2, 8, 1024), BF),
        vm((NY, 8, 1024), F32),
        vm((NZ, 448, 128), BF),
        vm((2, 4, 448, 128), BF),
        vm((8, 1024), F32),
        vm((16, 8, 128), F32),
        vm((NZ * NY, 8, 128), F32),
        vm((NY, 8, 128), F32),
        vm((8, 128), F32),
        dma((8,)),
        dma((13,)),
        dma((3, 2, 4, 2)),
        dma((2, 2, 2, 2)),
        dma((2,)),
        dma((2, 4)),
        dma((2,)),
        dma((2,)),
        dma((2,)),
        dma((2, 2, 2)),
        dma((4,)),
        dma((4,)),
        dma((1,)),
        dma((2, 4, 2)),
        dma((1,)),
        dma((1,)),
        dma((1,)),
    ]
    hbm = pl.BlockSpec(memory_space=pl.ANY)
    shapes = (
        jax.ShapeDtypeStruct((8, 4096), BF),
        jax.ShapeDtypeStruct((32, 128), F32),
        jax.ShapeDtypeStruct((448, 128), BF),
    )
    results = pl.pallas_call(
        kernel,
        out_shape=shapes,
        in_specs=[hbm] * 8,
        out_specs=(hbm,) * 3,
        scratch_shapes=scratch,
        compiler_params=pltpu.CompilerParams(
            collective_id=0, has_side_effects=True, vmem_limit_bytes=60 * 1024 * 1024
        ),
    )(
        tokens_in, grad_out, gate_pre.T, up_pre.T, gate_weight.T, up_weight.T, down_weight,
        norm_gain.reshape(32, 128),
    )
    igrad, ggrad, dgrad = pl.pallas_call(
        hand_on,
        out_shape=shapes,
        in_specs=[hbm] * 3,
        out_specs=(hbm,) * 3,
        scratch_shapes=[vm(v.shape, v.dtype) for v in shapes] + [dma((2, 3))],
        compiler_params=pltpu.CompilerParams(vmem_limit_bytes=60 * 1024 * 1024),
    )(*results)
    return igrad, ggrad.reshape(4096), dgrad


def solution(mesh):
    finer = Mesh(mesh.devices.reshape(NZ, NY, NX, 2, 2), AXES)
    return jax.shard_map(
        per_device,
        mesh=finer,
        in_specs=(
            P(AXES, None),
            P(AXES, None),
            P(DP, TENSOR),
            P(DP, TENSOR),
            P(DP, TENSOR),
            P(DP, TENSOR),
            P(TENSOR, DP),
            P(),
        ),
        out_specs=(P(AXES, None), P(), P(TENSOR, DP)),
        check_vma=False,
    )
```

```python
import jax
import jax.numpy as jnp
from jax import lax
from jax.experimental import pallas as pl
from jax.experimental.pallas import tpu as pltpu
from jax.sharding import Mesh
from jax.sharding import PartitionSpec as P

AXES = ("dp_0", "dp_1", "tensor_0", "tensor_1", "tensor_2")
Z, YH, X, YL, C = AXES
TENSOR = AXES[2:]
DP = AXES[:2]
BF = jnp.bfloat16
F32 = jnp.float32
MESH = pl.DeviceIdType.MESH
NZ, NY, NX = 8, 4, 4


def dot(a, b, ca, cb):
    return lax.dot_general(a, b, (((ca,), (cb,)), ((), ())), preferred_element_type=F32)


def kernel(
    tok_h, gout_h, gate_h, up_h, gw_h, uw_h, dw_h, gain_h,
    igrad, ggrad, dgrad,
    tok, gout, gain,
    w, gu, a, st, fac, act, sa, ra, rb, part, ga, pn, rc, sx, rx, fs, fn, gn, ds_, rd, gacc,
    g1, g3, g4, irms,
    lsem, ssem, wsem, gsem, s1sem, xsem, csem, rasem, rbsem, gasem, rcsem, rxsem, fnsem, rdsem,
    g1sem, g3sem, g4sem,
):
    z, k, x = lax.axis_index(Z), lax.axis_index(YH), lax.axis_index(X)
    yl, c = lax.axis_index(YL), lax.axis_index(C)
    sends = []

    def send(src, dst, dev, rsem, group):
        if group not in sends:
            sends.append(group)
        pltpu.make_async_remote_copy(
            src_ref=src, dst_ref=dst, send_sem=ssem.at[sends.index(group)], recv_sem=rsem,
            device_id=dev, device_id_type=MESH,
        ).start()

    def arrived(ref, rsem):
        pltpu.make_async_copy(ref, ref, rsem).wait()

    def units(n):
        return a.at[0].reshape(512, 1024).at[pl.ds(0, 8 * n)]

    def zz(d):
        return lax.rem(z + d + NZ, NZ)

    def yy(d):
        return lax.rem(k + d + NY, NY)

    def xx(d):
        return lax.rem(x + d + NX, NX)

    def ee(v, e):
        return lax.rem(v + e, 2)

    ys = [(d, e) for d in (2, 1, 3, 0) for e in (1, 0) if d or e]
    zs = (4, 3, 5, 2, 6, 1, 7, 0)
    dps = [(d, e) for d in zs for e in (2, 1, 3, 0) if d or e]
    ts = [(d, e, f) for d in (2, 1, 3, 0) for e in (1, 0) for f in (1, 0) if d or e or f]

    def ts_dev(d, e, f):
        return {X: xx(d), YL: ee(yl, e), C: ee(c, f)}

    def t_of(xs, ls, cs):
        return xs * 4 + ls * 2 + cs

    def ys_dev(d, e):
        return {YH: yy(d), YL: ee(yl, e)}

    peers = [{Z: zz(1)}, {Z: zz(-1)}] + [ys_dev(d, e) for d, e in ys]
    peers += [{X: xx(d)} for d in (2, 1, 3)] + [{C: 1 - c}]
    loads = [
        (gout_h, gout), (tok_h, tok), (dw_h, w.at[0, z]), (gate_h, gu.at[0, k]),
        (up_h, gu.at[1, k]), (gw_h, w.at[1, z]), (uw_h, w.at[2, z]), (gain_h, gain),
    ]
    loads = [pltpu.make_async_copy(s, d, lsem.at[i]) for i, (s, d) in enumerate(loads)]
    for i in (0, 2, 3, 4, 1, 5, 6, 7):
        loads[i].start()
    barrier = pltpu.get_barrier_semaphore()
    for p in peers:
        pl.semaphore_signal(barrier, inc=1, device_id=p, device_id_type=MESH)

    loads[0].wait()
    for q in range(NY):
        for i in range(NZ):
            col = (i * NY + q) * 128
            st[0, q, :, i * 128:(i + 1) * 128] = gout[:, col:col + 128]
    loads[2].wait()
    pl.semaphore_wait(barrier, len(peers))

    def half(ref, h):
        return ref.at[pl.ds(224 * h, 224)]

    class Ring:
        def __init__(self, buf, at, me, n, left, right, sem, group):
            self.buf, self.at, self.me, self.n, self.sem, self.group = buf, at, me, n, sem, group
            self.devs = (right, left)

        def put(self, slot, way, step, h):
            p = half(self.buf.at[slot], h)
            send(p, p, self.devs[way], self.sem.at[way, step, h], self.group)

        def first(self):
            for i in range(2):
                for way in range(2):
                    self.put(self.me, way, 0, i ^ way)

        def got(self, s, way, h):
            slot = self.at(-s if way == 0 else s)
            arrived(half(self.buf.at[slot], h), self.sem.at[way, s - 1, h])
            return slot

        def nxt(self, s, parts=(0, 1)):
            for i in parts:
                for way in range(2):
                    slot = self.got(s, way, i ^ way)
                    if s + 1 < self.n // 2 or i == 0:
                        self.put(slot, way, s, i ^ way)

        def last(self):
            for way in range(2):
                self.got(self.n // 2, way, way)

    zl, zr, kl, kr = {Z: zz(-1)}, {Z: zz(1)}, {YH: yy(-1)}, {YH: yy(1)}
    dwr, gwr, uwr = [Ring(w.at[i], zz, z, NZ, zl, zr, wsem.at[i], "w%d" % i) for i in range(3)]
    gater, upr = [Ring(gu.at[i], yy, k, NY, kl, kr, gsem.at[i], "gu") for i in range(2)]
    gar = Ring(ga, yy, k, NY, kl, kr, gasem, "ga")
    core = {C: 1 - c}

    def s1_send(i):
        for d, e in ys:
            send(st.at[i, yy(d)], a.at[i, k, x, yl, c], ys_dev(d, e), s1sem.at[i], "s1")

    def s1_wait(i):
        arrived(units(7), s1sem.at[i])

    def unit(i, xs, cs):
        return a.at[i, :, xs, :, cs]

    def x_send(i):
        for d in (2, 1, 3):
            send(unit(i, x, c), unit(i, x, c), {X: xx(d)}, xsem.at[i, d], "x%d" % i)
        send(unit(i, x, c), unit(i, x, c), core, csem.at[i], "x%d" % i)

    def x_wait(i):
        for d in (1, 3, 2):
            u = unit(i, xx(-d), c)
            arrived(u, xsem.at[i, d])
            send(u, u, core, csem.at[i], "x%d" % i)

    def core_wait(i):
        arrived(units(32), csem.at[i])

    dwr.first()
    s1_send(0)
    for cp in loads[3:5]:
        cp.wait()
    gater.first()
    upr.first()
    a[0, k, x, yl, c] = st[0, k]

    loads[1].wait()
    tf = tok[...].astype(F32)
    inv = lax.rsqrt(jnp.mean(tf * tf, axis=1, keepdims=True) + 1e-05)
    irms[...] = jnp.broadcast_to(inv, (8, 128))
    for q in range(NY):
        for i in range(NZ):
            col = (i * NY + q) * 128
            st[1, q, :, i * 128:(i + 1) * 128] = (tf[:, col:col + 128] * inv).astype(BF)
    a[1, k, x, yl, c] = st[1, k]
    s1_send(1)
    for cp in loads[5:]:
        cp.wait()

    dwr.nxt(1)
    s1_wait(0)
    x_send(0)
    dwr.nxt(2)
    dwr.nxt(3, (0,))
    gwr.first()
    uwr.first()
    x_wait(0)
    dwr.nxt(3, (1,))
    dwr.last()
    gater.nxt(1, (0,))
    core_wait(0)

    down = jnp.concatenate([w[0, i] for i in range(NZ)], axis=1)

    def partial(d, e):
        rows = [a.at[0, yy(v)].reshape(128, 1024)[...] for v in (d, e)]
        both = dot(down, jnp.concatenate(rows, axis=0), 1, 1)
        return both[:, :128], both[:, 128:]

    def own_half(n, dev, h):
        rows = slice(224 * h, 224 * h + 224)
        sa[2 * n, rows] = part[n, rows].astype(BF)
        send(half(sa.at[2 * n], h), half(ra.at[n], h), dev, rasem.at[n], "ga")

    far, part[0] = partial(2, 1)
    sa[1] = far.astype(BF)
    send(half(sa.at[1], 0), rb.at[0], kr, rbsem.at[0], "ga")
    send(half(sa.at[1], 1), rb.at[1], kl, rbsem.at[1], "ga")
    own_half(0, kr, 1)
    part[1], part[2] = partial(3, 0)
    own_half(1, kl, 0)

    gwr.nxt(1)
    uwr.nxt(1)
    s1_wait(1)
    x_send(1)

    for n, (dev, h) in enumerate(((kr, 0), (kl, 1))):
        rows = slice(224 * h, 224 * h + 224)
        arrived(rb.at[n], rbsem.at[n])
        sa[2 * n, rows] = (part[n, rows] + rb[n].astype(F32)).astype(BF)
        send(half(sa.at[2 * n], h), half(ra.at[n], h), dev, rasem.at[n], "ga")
    upr.nxt(1, (0,))
    gwr.nxt(2)
    uwr.nxt(2)
    x_wait(1)
    gwr.nxt(3, (0,))
    for n in range(2):
        arrived(ra.at[n], rasem.at[n])
    ga[k] = (part[2] + ra[0].astype(F32) + ra[1].astype(F32)).astype(BF)
    gar.first()

    gater.nxt(1, (1,))
    gater.last()
    upr.nxt(1, (1,))
    upr.last()
    for j in range(NY):
        gv = gu[0, j].astype(F32)
        uv = gu[1, j].astype(F32)
        sg = jax.nn.sigmoid(gv)
        sv = gv * sg
        fac[0, j] = uv * sg * (1.0 + gv * (1.0 - sg))
        fac[1, j] = sv
        act[j] = (sv * uv).astype(BF)
    uwr.nxt(3, (0,))

    acts = jnp.concatenate([act[j] for j in range(NY)], axis=1)
    rows_all = a.at[0].reshape(512, 1024)
    for i in range(NZ // 2):
        pair = dot(acts, rows_all[:, i * 256:(i + 1) * 256], 1, 0)
        ds_[2 * i] = pair[:, :128].astype(BF)
        ds_[2 * i + 1] = pair[:, 128:].astype(BF)

    def down_put(way, slot, step, h):
        send(
            half(ds_.at[slot], h), half(rd.at[way, step], h), (zr, zl)[way],
            rdsem.at[way, step, h], "down",
        )

    def down_add(way, slot, step, h):
        arrived(half(rd.at[way, step], h), rdsem.at[way, step, h])
        rows = slice(224 * h, 224 * h + 224)
        ds_[slot, rows] = (
            ds_[slot, rows].astype(F32) + rd[way, step, rows].astype(F32)
        ).astype(BF)

    def down_next(s, i):
        for way in range(2):
            slot = zz(4 - s if way == 0 else s - 4)
            down_add(way, slot, s - 1, i ^ way)
            if s < 4:
                down_put(way, slot, s, i ^ way)

    for way in range(2):
        down_put(way, zz(4), 0, way)
    for way in range(2):
        down_put(way, zz(3 if way == 0 else -3), 1, 1 - way)

    def norm_part(d):
        j = yy(-d)
        gj = ga[j].astype(F32)
        both = jnp.concatenate([(gj * fac[0, j]).astype(BF), (gj * fac[1, j]).astype(BF)], axis=0)
        for i in range(NZ // 2):
            cols = jnp.concatenate(
                [
                    jnp.concatenate([w[1, 2 * i], w[2, 2 * i]], axis=0),
                    jnp.concatenate([w[1, 2 * i + 1], w[2, 2 * i + 1]], axis=0),
                ],
                axis=1,
            )
            block = dot(both, cols, 0, 0)
            lanes = slice(i * 256, (i + 1) * 256)
            for q in range(16):
                pn[d, q // 4, (q // 2) % 2, q % 2, :, lanes] = block[q * 8:(q + 1) * 8].astype(BF)
        send(pn.at[d, :, :, 1 - c], rc.at[d], core, rcsem.at[d], "norm")

    def norm_core(d):
        arrived(rc.at[d], rcsem.at[d])
        for i in range(NX):
            for j in range(2):
                sx[d, i, j] = (pn[d, i, j, c].astype(F32) + rc[d, i, j].astype(F32)).astype(BF)
        for e in (2, 1, 3):
            send(sx.at[d, xx(e)], rx.at[d, e], {X: xx(e)}, rxsem.at[d], "norm")

    def norm_x(d):
        arrived(units(6), rxsem.at[d])
        for f in (1, 0):
            v = ee(yl, f)
            rows = sx[d, x, v].astype(F32)
            for e in range(1, NX):
                rows = rows + rx[d, e, v].astype(F32)
            if d or f:
                fs[d, f] = rows.astype(BF)
                send(fs.at[d, f], fn.at[k, yl], ys_dev(-d, f), fnsem.at[0], "norm")
            else:
                fn[k, yl] = rows.astype(BF)

    def gain_part(d):
        add = gacc[...]
        for q in range(16):
            at = (q // 4, (q // 2) % 2, q % 2)
            add = add + pn[(d,) + at].astype(F32) * a[(1, yy(-d)) + at].astype(F32)
        gacc[...] = add

    gacc[...] = jnp.zeros((8, 1024), F32)
    gar.nxt(1, (0,))
    gwr.nxt(3, (1,))
    gwr.last()
    uwr.nxt(3, (1,))
    uwr.last()
    norm_part(0)
    gar.nxt(1, (1,))
    norm_part(1)
    norm_part(3)
    norm_core(0)
    norm_core(1)
    down_next(1, 0)
    down_next(2, 1)
    core_wait(1)
    for d in (0, 1, 3):
        gain_part(d)
    gar.last()
    norm_part(2)

    gain_part(2)
    mine = t_of(x, yl, c)
    for i in range(NZ):
        g1[mine, i:i + 1, :] = jnp.sum(gacc[:, i * 128:(i + 1) * 128], axis=0, keepdims=True)
    for d, e, f in ts:
        send(g1.at[mine], g1.at[mine], ts_dev(d, e, f), g1sem.at[0], "g1")

    norm_core(2)
    norm_core(3)
    down_next(2, 0)
    down_next(3, 1)
    norm_x(0)
    norm_x(1)
    arrived(g1.at[pl.ds(0, 15)], g1sem.at[0])

    @pl.when(c == 1)
    def _():
        g3[z * NY + k] = jnp.sum(g1[...], axis=0)
        for d, e in dps:
            send(
                g3.at[z * NY + k], g3.at[z * NY + k], {Z: zz(d), YH: yy(e)}, g3sem.at[0], "g3"
            )

    norm_x(2)
    norm_x(3)
    down_next(3, 0)
    down_next(4, 1)


    down_next(4, 0)
    outs = [pltpu.make_async_copy(ds_.at[z], dgrad, lsem.at[0])]
    outs[0].start()

    arrived(units(7), fnsem.at[0])
    for q in range(NY):
        gn[q] = fn[q, 0].astype(F32) + fn[q, 1].astype(F32)
    inv = irms[...]
    inner = jnp.zeros((8, 128), F32)
    for i in range(NZ):
        for q in range(NY):
            b = i * NY + q
            normed = tok[:, b * 128:(b + 1) * 128].astype(F32) * inv
            inner = inner + gn[q, :, i * 128:(i + 1) * 128] * gain[b:b + 1, :] * normed
    inner = jnp.sum(inner, axis=1, keepdims=True) * (1.0 / 4096)
    for i in range(NZ):
        for q in range(NY):
            b = i * NY + q
            cols = slice(b * 128, (b + 1) * 128)
            normed = tok[:, cols].astype(F32) * inv
            scaled = gn[q, :, i * 128:(i + 1) * 128] * gain[b:b + 1, :]
            tok[:, cols] = (
                gout[:, cols].astype(F32) + inv * (scaled - normed * inner)
            ).astype(BF)

    outs.append(pltpu.make_async_copy(tok, igrad, lsem.at[1]))
    outs[1].start()

    @pl.when(c == 1)
    def _():
        arrived(g3.at[pl.ds(0, 31)], g3sem.at[0])
        for q in range(NY):
            total = g3[q]
            for i in range(1, NZ):
                total = total + g3[i * NY + q]
            g4[q] = total
        send(g4, ggrad, core, g4sem.at[0], "g4")
        mine = pltpu.make_async_copy(g4, ggrad, lsem.at[2])
        mine.start()
        mine.wait()

    @pl.when(c == 0)
    def _():
        arrived(g4, g4sem.at[0])

    sent = {
        "w0": w.at[0, pl.ds(0, 7)], "w1": w.at[0, pl.ds(0, 7)], "w2": w.at[0, pl.ds(0, 7)],
        "gu": w.at[0, pl.ds(0, 6)], "ga": w.at[0, pl.ds(0, 6)], "down": w.at[0, pl.ds(0, 7)],
        "s1": units(14), "x0": units(56), "x1": units(56), "norm": units(63),
        "g1": g1.at[pl.ds(0, 15)], "g3": g3.at[pl.ds(0, 31)], "g4": g4,
    }

    def all_sent(late):
        for i, group in enumerate(sends):
            if (group in ("g3", "g4")) == late:
                arrived(sent[group], ssem.at[i])

    all_sent(False)

    @pl.when(c == 1)
    def _():
        all_sent(True)

    for cp in outs:
        cp.wait()


def hand_on(i0, i1, i2, o0, o1, o2, b0, b1, b2, rows, sem):
    ins = [pltpu.make_async_copy(s, d, sem.at[0, n]) for n, (s, d) in enumerate(((i0, b0), (i1, b1), (i2, b2)))]
    outs = [pltpu.make_async_copy(s, d, sem.at[1, n]) for n, (s, d) in enumerate(((b0, o0), (rows, o1), (b2, o2)))]
    for cp in ins:
        cp.start()
    ins[1].wait()
    for i in range(NZ):
        for q in range(NY):
            b = i * NY + q
            rows[b:b + 1, :] = b1[q, i:i + 1, :]
    outs[1].start()
    for n in (0, 2):
        ins[n].wait()
        outs[n].start()
    for cp in outs:
        cp.wait()


def per_device(
    tokens_in, grad_out, gate_pre, up_pre, gate_weight, up_weight, down_weight, norm_gain
):
    vm = pltpu.VMEM
    dma = pltpu.SemaphoreType.DMA
    scratch = [
        vm((8, 4096), BF),
        vm((8, 4096), BF),
        vm((32, 128), F32),
        vm((3, NZ, 448, 128), BF),
        vm((2, NY, 448, 128), BF),
        vm((2, NY, NX, 2, 2, 8, 1024), BF),
        vm((2, NY, 8, 1024), BF),
        vm((2, NY, 448, 128), F32),
        vm((NY, 448, 128), BF),
        vm((3, 448, 128), BF),
        vm((2, 448, 128), BF),
        vm((2, 224, 128), BF),
        vm((3, 448, 128), F32),
        vm((NY, 448, 128), BF),
        vm((NY, NX, 2, 2, 8, 1024), BF),
        vm((NY, NX, 2, 8, 1024), BF),
        vm((NY, NX, 2, 8, 1024), BF),
        vm((NY, NX, 2, 8, 1024), BF),
        vm((NY, 2, 8, 1024), BF),
        vm((NY, 2, 8, 1024), BF),
        vm((NY, 8, 1024), F32),
        vm((NZ, 448, 128), BF),
        vm((2, 4, 448, 128), BF),
        vm((8, 1024), F32),
        vm((16, 8, 128), F32),
        vm((NZ * NY, 8, 128), F32),
        vm((NY, 8, 128), F32),
        vm((8, 128), F32),
        dma((8,)),
        dma((13,)),
        dma((3, 2, 4, 2)),
        dma((2, 2, 2, 2)),
        dma((2,)),
        dma((2, 4)),
        dma((2,)),
        dma((2,)),
        dma((2,)),
        dma((2, 2, 2)),
        dma((4,)),
        dma((4,)),
        dma((1,)),
        dma((2, 4, 2)),
        dma((1,)),
        dma((1,)),
        dma((1,)),
    ]
    hbm = pl.BlockSpec(memory_space=pl.ANY)
    shapes = (
        jax.ShapeDtypeStruct((8, 4096), BF),
        jax.ShapeDtypeStruct((32, 128), F32),
        jax.ShapeDtypeStruct((448, 128), BF),
    )
    results = pl.pallas_call(
        kernel,
        out_shape=(shapes[0], jax.ShapeDtypeStruct((NY, 8, 128), F32), shapes[2]),
        in_specs=[hbm] * 8,
        out_specs=(hbm,) * 3,
        scratch_shapes=scratch,
        compiler_params=pltpu.CompilerParams(
            collective_id=0, has_side_effects=True, vmem_limit_bytes=60 * 1024 * 1024
        ),
    )(
        tokens_in, grad_out, gate_pre.T, up_pre.T, gate_weight.T, up_weight.T, down_weight,
        norm_gain.reshape(32, 128),
    )
    igrad, ggrad, dgrad = pl.pallas_call(
        hand_on,
        out_shape=shapes,
        in_specs=[hbm] * 3,
        out_specs=(hbm,) * 3,
        scratch_shapes=[
            vm((8, 4096), BF), vm((NY, 8, 128), F32), vm((448, 128), BF), vm((32, 128), F32),
            dma((2, 3)),
        ],
        compiler_params=pltpu.CompilerParams(vmem_limit_bytes=60 * 1024 * 1024),
    )(*results)
    return igrad, ggrad.reshape(4096), dgrad


def solution(mesh):
    finer = Mesh(mesh.devices.reshape(NZ, NY, NX, 2, 2), AXES)
    return jax.shard_map(
        per_device,
        mesh=finer,
        in_specs=(
            P(AXES, None),
            P(AXES, None),
            P(DP, TENSOR),
            P(DP, TENSOR),
            P(DP, TENSOR),
            P(DP, TENSOR),
            P(TENSOR, DP),
            P(),
        ),
        out_specs=(P(AXES, None), P(), P(TENSOR, DP)),
        check_vma=False,
    )
```
